32 devices in a mesh: dp: 1 (over z), seq: 32 (over y, x, core).
Axes of the slice: x: 4, y: 4, z: 1, core: 2. Of those that a mesh axis runs over, the one named last changes fastest.
The devices are a block of a 4x4x8 slice.
Arguments:
- enc_out: bfloat16 [32, 64, 1024], P('dp', 'seq')
- pred_out: bfloat16 [32, 64, 640], P('dp')
- w_enc: bfloat16 [1024, 640], replicated
- w_pred: bfloat16 [640, 640], replicated
- w_out: bfloat16 [640, 1024], replicated
- labels: int32 [32, 63], P('dp')
- frame_len: int32 [32], P('dp')
- label_len: int32 [32], P('dp')
Outputs:
- output 1: float32 [32], P('dp')
- output 2: bfloat16 [32, 64, 1024], P('dp', 'seq')
- output 3: float32 [1024, 640], P('dp')
- output 4: float32 [640, 640], P('dp')
- output 5: float32 [640, 1024], P('dp')
All inputs are finite; a program needn't handle non-finite values.
Results may differ from the reference program's by a relative error of at most 0.0138273.
Values are sent between devices in bfloat16 or wider.
A program may use at most 768 MiB of HBM per device.

```python
import jax
import jax.numpy as jnp
from jax import lax

NUM_UTT = 32
NUM_FRAMES = 64
LABEL_POS = 64
ENC_DIM = 1024
PRED_DIM = 640
JOINT_DIM = 640
VOCAB_SIZE = 1024
FRAME_BLOCK = 2
NUM_LABELS = LABEL_POS - 1
NUM_BLOCKS = NUM_FRAMES // FRAME_BLOCK
NEG_FILL = -1.0e30


def setup_inputs(seed: int = 0, part: int = 0) -> dict:
    shared_key, part_base = jax.random.split(jax.random.key(seed))
    part_key = jax.random.fold_in(part_base, part)
    k_enc, k_pred, k_lab, k_frames, k_lens = jax.random.split(part_key, 5)
    k_wenc, k_wpred, k_wout = jax.random.split(shared_key, 3)
    enc_out = jax.random.normal(k_enc, (NUM_UTT, NUM_FRAMES, ENC_DIM), jnp.float32).astype(jnp.bfloat16)
    pred_out = jax.random.normal(k_pred, (NUM_UTT, LABEL_POS, PRED_DIM), jnp.float32).astype(jnp.bfloat16)
    w_enc = (jax.random.normal(k_wenc, (ENC_DIM, JOINT_DIM), jnp.float32) * ENC_DIM ** -0.5).astype(jnp.bfloat16)
    w_pred = (jax.random.normal(k_wpred, (PRED_DIM, JOINT_DIM), jnp.float32) * PRED_DIM ** -0.5).astype(jnp.bfloat16)
    w_out = (jax.random.normal(k_wout, (JOINT_DIM, VOCAB_SIZE), jnp.float32) * (1.5 * JOINT_DIM ** -0.5)).astype(jnp.bfloat16)
    labels = jax.random.randint(k_lab, (NUM_UTT, NUM_LABELS), 1, VOCAB_SIZE, jnp.int32)
    frame_len = jax.random.randint(k_frames, (NUM_UTT,), NUM_FRAMES // 4 + 1, NUM_FRAMES + 1, jnp.int32).at[0].set(NUM_FRAMES)
    label_len = jax.random.randint(k_lens, (NUM_UTT,), 1, NUM_LABELS + 1, jnp.int32).at[NUM_UTT - 1].set(NUM_LABELS)
    return {'enc_out': enc_out, 'pred_out': pred_out, 'w_enc': w_enc, 'w_pred': w_pred, 'w_out': w_out, 'labels': labels, 'frame_len': frame_len, 'label_len': label_len}


def joint_block(enc_blk, act_g, w_enc, w_out):
    n_utt, n_blk, _ = enc_blk.shape
    act_f = jnp.dot(enc_blk.reshape(n_utt * n_blk, ENC_DIM), w_enc, preferred_element_type=jnp.float32).astype(jnp.bfloat16).reshape(n_utt, n_blk, JOINT_DIM)
    hidden = jnp.tanh(act_f[:, :, None, :].astype(jnp.float32) + act_g[:, None, :, :].astype(jnp.float32)).astype(jnp.bfloat16)
    logits = jnp.dot(hidden.reshape(n_utt * n_blk * LABEL_POS, JOINT_DIM), w_out, preferred_element_type=jnp.float32).reshape(n_utt, n_blk, LABEL_POS, VOCAB_SIZE)
    return hidden, jax.nn.log_softmax(logits, axis=-1)


def label_prefix(frame_lab):
    zero_col = jnp.zeros_like(frame_lab[:, :1])
    return jnp.concatenate([zero_col, jnp.cumsum(frame_lab, axis=1)], axis=1)


def reference(enc_out, pred_out, w_enc, w_pred, w_out, labels, frame_len, label_len):
    act_g = jnp.dot(pred_out.reshape(NUM_UTT * LABEL_POS, PRED_DIM), w_pred, preferred_element_type=jnp.float32).astype(jnp.bfloat16).reshape(NUM_UTT, LABEL_POS, JOINT_DIM)
    lab_ids = jnp.concatenate([labels, jnp.full((NUM_UTT, 1), -1, jnp.int32)], axis=1)
    lab_index = jnp.broadcast_to(labels[:, None, :, None], (NUM_UTT, FRAME_BLOCK, NUM_LABELS, 1))
    enc_blocks = enc_out.reshape(NUM_UTT, NUM_BLOCKS, FRAME_BLOCK, ENC_DIM).transpose(1, 0, 2, 3)

    def lattice_scores(enc_blk):
        _, log_probs = joint_block(enc_blk, act_g, w_enc, w_out)
        lab_lp = jnp.take_along_axis(log_probs[:, :, :NUM_LABELS, :], lab_index, axis=3)[..., 0]
        return log_probs[..., 0], lab_lp

    blank_blocks, lab_blocks = lax.map(lattice_scores, enc_blocks)
    blank_lp = blank_blocks.transpose(1, 0, 2, 3).reshape(NUM_UTT, NUM_FRAMES, LABEL_POS)
    lab_lp = lab_blocks.transpose(1, 0, 2, 3).reshape(NUM_UTT, NUM_FRAMES, NUM_LABELS)

    pos_ids = jnp.arange(LABEL_POS)[None, :]
    neg_rows = jnp.full((NUM_UTT, LABEL_POS), NEG_FILL, jnp.float32)
    init_x = jnp.where(pos_ids == 0, 0.0, neg_rows)
    boundary = jnp.where(pos_ids == label_len[:, None], 0.0, neg_rows)

    def alpha_step(x_prev, frame_in):
        frame_blank, frame_lab = frame_in
        lab_sum = label_prefix(frame_lab)
        alpha_t = lab_sum + lax.cumlogsumexp(x_prev - lab_sum, axis=1)
        return alpha_t + frame_blank, alpha_t

    _, alphas = lax.scan(alpha_step, init_x, (blank_lp.transpose(1, 0, 2), lab_lp.transpose(1, 0, 2)))
    alphas = alphas.transpose(1, 0, 2)

    def beta_step(next_row, frame_in):
        frame_blank, frame_lab, frame_id = frame_in
        lab_sum = label_prefix(frame_lab)
        beta_row = lax.cumlogsumexp(next_row + frame_blank + lab_sum, axis=1, reverse=True) - lab_sum
        beta_row = jnp.where((frame_id >= frame_len)[:, None], boundary, beta_row)
        return beta_row, (beta_row, next_row)

    first_row, (betas, beta_next) = lax.scan(beta_step, boundary, (blank_lp.transpose(1, 0, 2), lab_lp.transpose(1, 0, 2), jnp.arange(NUM_FRAMES)), reverse=True)
    betas = betas.transpose(1, 0, 2)
    beta_next = beta_next.transpose(1, 0, 2)
    log_prob = first_row[:, 0]

    beta_up = jnp.concatenate([betas[:, :, 1:], jnp.full((NUM_UTT, NUM_FRAMES, 1), NEG_FILL, jnp.float32)], axis=2)
    lab_full = jnp.concatenate([lab_lp, jnp.zeros((NUM_UTT, NUM_FRAMES, 1), jnp.float32)], axis=2)
    frame_ok = (jnp.arange(NUM_FRAMES)[None, :] < frame_len[:, None])[:, :, None]
    norm_shift = log_prob[:, None, None]
    occ_blank = jnp.where(frame_ok, jnp.exp(jnp.minimum(alphas + blank_lp + beta_next - norm_shift, 0.0)), 0.0)
    occ_lab = jnp.where(frame_ok, jnp.exp(jnp.minimum(alphas + lab_full + beta_up - norm_shift, 0.0)), 0.0)

    def to_blocks(arr):
        return arr.reshape(NUM_UTT, NUM_BLOCKS, FRAME_BLOCK, LABEL_POS).transpose(1, 0, 2, 3)

    vocab_ids = jnp.arange(VOCAB_SIZE)

    def grad_step(acc_carry, blk_in):
        gw_enc, gw_out, d_act_g = acc_carry
        enc_blk, occ_b, occ_l = blk_in
        hidden, log_probs = joint_block(enc_blk, act_g, w_enc, w_out)
        d_logits = (jnp.exp(log_probs) * (occ_b + occ_l)[..., None] - jnp.where(vocab_ids == 0, occ_b[..., None], 0.0) - jnp.where(vocab_ids == lab_ids[:, None, :, None], occ_l[..., None], 0.0)).astype(jnp.bfloat16)
        flat_dz = d_logits.reshape(NUM_UTT * FRAME_BLOCK * LABEL_POS, VOCAB_SIZE)
        flat_h = hidden.reshape(NUM_UTT * FRAME_BLOCK * LABEL_POS, JOINT_DIM)
        d_hidden = jnp.dot(flat_dz, w_out.T, preferred_element_type=jnp.float32)
        d_pre = (d_hidden * (1.0 - jnp.square(flat_h.astype(jnp.float32)))).astype(jnp.bfloat16).reshape(NUM_UTT, FRAME_BLOCK, LABEL_POS, JOINT_DIM)
        d_act_f = jnp.sum(d_pre.astype(jnp.float32), axis=2).astype(jnp.bfloat16).reshape(NUM_UTT * FRAME_BLOCK, JOINT_DIM)
        grad_blk = jnp.dot(d_act_f, w_enc.T, preferred_element_type=jnp.float32).astype(jnp.bfloat16).reshape(NUM_UTT, FRAME_BLOCK, ENC_DIM)
        gw_enc = gw_enc + jnp.dot(enc_blk.reshape(NUM_UTT * FRAME_BLOCK, ENC_DIM).T, d_act_f, preferred_element_type=jnp.float32)
        gw_out = gw_out + jnp.dot(flat_h.T, flat_dz, preferred_element_type=jnp.float32)
        d_act_g = d_act_g + jnp.sum(d_pre.astype(jnp.float32), axis=1)
        return (gw_enc, gw_out, d_act_g), grad_blk

    acc_init = (jnp.zeros((ENC_DIM, JOINT_DIM), jnp.float32), jnp.zeros((JOINT_DIM, VOCAB_SIZE), jnp.float32), jnp.zeros((NUM_UTT, LABEL_POS, JOINT_DIM), jnp.float32))
    (gw_enc, gw_out, d_act_g), grad_blocks = lax.scan(grad_step, acc_init, (enc_blocks, to_blocks(occ_blank), to_blocks(occ_lab)))
    grad_enc = grad_blocks.transpose(1, 0, 2, 3).reshape(NUM_UTT, NUM_FRAMES, ENC_DIM)
    gw_pred = jnp.einsum('buh,buj->hj', pred_out.astype(jnp.float32), d_act_g.astype(jnp.float32))
    return -log_prob, grad_enc, gw_enc, gw_pred, gw_out
```

```python
import functools

import jax
import jax.numpy as jnp
from jax import lax
from jax.experimental import pallas as pl
from jax.experimental.pallas import tpu as pltpu
from jax.sharding import PartitionSpec as P

NEG = -1.0e30
SIDE = 4
LANES = 128
BLK_T = 8
F32 = jnp.float32
BF16 = jnp.bfloat16


def dot(a, b, ca, cb):
    return lax.dot_general(a, b, (((ca,), (cb,)), ((), ())), preferred_element_type=F32)


def lse2(x, y):
    m = jnp.maximum(x, y)
    return m + jnp.log(1.0 + jnp.exp(-jnp.abs(x - y)))


def pieces_rows(rows, cols, parts):
    tiles = rows * cols // (8 * LANES)
    return -(-tiles // parts) * 8


class Comm:
    def __init__(self, send_sem, recv_sem):
        self.send_sem, self.recv_sem, self.used, self.sent = send_sem, recv_sem, 0, []

    def send(self, src, dst, dev):
        k = self.used
        self.used += 1
        cp = pltpu.make_async_remote_copy(src_ref=src, dst_ref=dst, send_sem=self.send_sem.at[k], recv_sem=self.recv_sem.at[k],
                                          device_id={'seq': dev}, device_id_type=pl.DeviceIdType.MESH)
        cp.start()
        self.sent.append(cp)
        return cp

    def drain(self):
        for cp in self.sent:
            cp.wait_send()
        self.sent = []


class Ring:
    def __init__(self, pos, dev_of):
        self.me, self.r, self.l, self.o = pos, (pos + 1) % SIDE, (pos + 3) % SIDE, (pos + 2) % SIDE
        self.right, self.left = dev_of(self.r), dev_of(self.l)


def rs_start(comm, ring, view, buf):
    return (comm.send(view(ring.o, 0), buf[0], ring.right), comm.send(view(ring.o, 1), buf[2], ring.left),
            comm.send(view(ring.r, 1), buf[1], ring.right), comm.send(view(ring.l, 0), buf[3], ring.left))


def rs_mid(comm, ring, view, buf, st):
    st[0].wait_recv()
    v = view(ring.r, 0)
    v[...] += buf[0][...]
    a = comm.send(v, buf[4], ring.right)
    st[1].wait_recv()
    v = view(ring.l, 1)
    v[...] += buf[2][...]
    b = comm.send(v, buf[5], ring.left)
    return st + (a, b)


def rs_end(ring, view, buf, st, out):
    for k in (2, 3, 4, 5):
        st[k].wait_recv()
    out(0, view(ring.me, 0)[...] + buf[4][...] + buf[3][...])
    out(1, view(ring.me, 1)[...] + buf[5][...] + buf[1][...])


def ag_start(comm, ring, whole):
    v = whole(ring.me)
    return (comm.send(v, v, ring.right), comm.send(v, v, ring.left))


def ag_mid(comm, ring, half, st):
    st[0].wait_recv()
    v = half(ring.l, 0)
    a = comm.send(v, v, ring.right)
    st[1].wait_recv()
    v = half(ring.r, 1)
    b = comm.send(v, v, ring.left)
    return (a, b)


def ag_end(st):
    st[0].wait_recv()
    st[1].wait_recv()


class AllReduce:
    def __init__(self, comm, pos, part, full, r0, r1, r2):
        self.comm, (self.core, x, y, dev) = comm, pos
        self.part, self.full, self.r0, self.r1, self.r2 = part, full, r0, r1, r2
        rx = Ring(x, lambda i: dev(i, y, self.core))
        ry = Ring(y, lambda i: dev(x, i, self.core))
        self.rings = ((rx, ry), (ry, rx))
        self.sibling = dev(x, y, 1 - self.core)
        n = part.shape[4]
        h = n // 16 * 8
        self.cut = ((0, h), (h, n - h))

    def v1(self, ref, k):
        return lambda a, half: ref.at[self.core, k, a, pl.ds(2 * half, 2)]

    def v2(self, ref, k):
        return lambda b, half: ref.at[self.core, k, self.rings[k][0].me, b, pl.ds(*self.cut[half])]

    def b1(self, k):
        return [self.r1.at[k, s] for s in range(6)]

    def b2(self, k):
        return [self.r2.at[k, s, pl.ds(*self.cut[h])] for s, h in enumerate((0, 1, 1, 0, 0, 1))]

    def d2d_start(self):
        self.st0 = self.comm.send(self.part.at[1 - self.core], self.r0, self.sibling)

    def rs1_start(self):
        self.st0.wait_recv()
        self.part[pl.ds(self.core, 1)] += self.r0[...][None]
        self.st = [rs_start(self.comm, self.rings[k][0], self.v1(self.part, k), self.b1(k)) for k in range(2)]

    def rs1_mid(self):
        self.st = [rs_mid(self.comm, self.rings[k][0], self.v1(self.part, k), self.b1(k), self.st[k]) for k in range(2)]

    def rs2_start(self):
        for k in range(2):
            view = self.v1(self.part, k)

            def put(half, val, view=view, k=k):
                view(self.rings[k][0].me, half)[...] = val
            rs_end(self.rings[k][0], view, self.b1(k), self.st[k], put)
            self.st[k] = rs_start(self.comm, self.rings[k][1], self.v2(self.part, k), self.b2(k))

    def rs2_mid(self):
        self.st = [rs_mid(self.comm, self.rings[k][1], self.v2(self.part, k), self.b2(k), self.st[k]) for k in range(2)]

    def ag2_start(self):
        for k in range(2):
            dst = self.v2(self.full, k)

            def put(half, val, dst=dst, k=k):
                dst(self.rings[k][1].me, half)[...] = val
            rs_end(self.rings[k][1], self.v2(self.part, k), self.b2(k), self.st[k], put)
            self.st[k] = ag_start(self.comm, self.rings[k][1], lambda b, k=k: self.full.at[self.core, k, self.rings[k][0].me, b])

    def ag2_mid(self):
        self.st = [ag_mid(self.comm, self.rings[k][1], self.v2(self.full, k), self.st[k]) for k in range(2)]

    def ag1_start(self):
        for k in range(2):
            ag_end(self.st[k])
            self.st[k] = ag_start(self.comm, self.rings[k][0], lambda a, k=k: self.full.at[self.core, k, a])

    def ag1_mid(self):
        self.st = [ag_mid(self.comm, self.rings[k][0], self.v1(self.full, k), self.st[k]) for k in range(2)]

    def d2d_back(self):
        for k in range(2):
            ag_end(self.st[k])
        half = self.full.at[self.core]
        self.st0 = self.comm.send(half, half, self.sibling)

    def finish(self):
        self.st0.wait_recv()


STEPS = ('d2d_start', 'rs1_start', 'rs1_mid', 'rs2_start', 'rs2_mid', 'ag2_start', 'ag2_mid', 'ag1_start', 'ag1_mid', 'd2d_back', 'finish')


def skew(mat, sign):
    rows = lax.broadcasted_iota(jnp.int32, mat.shape, 0)
    bit = 1
    while bit < mat.shape[0]:
        amount = bit if sign > 0 else LANES - bit
        mat = jnp.where((rows & bit) != 0, pltpu.roll(mat, amount, 1), mat)
        bit *= 2
    return mat


def kernel(n, f_ref, pred_ref, we_ref, wp_ref, wo_ref, lab_ref, flen_ref, llen_ref,
           loss_ref, genc_ref, full_out, full_pred, full_enc,
           g_ref, abuf, a_ref, act_ref, c_ref, onehot_ref, h_ref, z_ref, e_ref, bt_ref, lt_ref, rs_ref,
           sb_ref, sl_ref, al_ref, be_ref, c1_ref, gb_ref, gl_ref, dz_ref, dc_ref, dabuf, darecv, daloc, lossbuf,
           p_out, p_pred, p_enc, r0o, r1o, r2o, r0p, r1p, r2p, r0e, r1e, r2e,
           gsem, asend, arecv, dsend, drecv, ssem, rsem):
    me = lax.axis_index('seq')
    core, x, y = me % 2, (me // 2) % SIDE, me // (2 * SIDE)

    def dev(i, j, c):
        return (j * SIDE + i) * 2 + c

    n_t, n_u, n_j, n_v = a_ref.shape[0], c_ref.shape[0], c_ref.shape[1], wo_ref.shape[1]
    tl = n_t // n
    rows = BLK_T * n_u
    n_blk = n_t // BLK_T

    gcopy = pltpu.make_async_copy(pred_ref.at[me], g_ref, gsem)
    gcopy.start()
    barrier = pltpu.get_barrier_semaphore()

    def greet(p, c):
        pl.semaphore_signal(barrier, inc=1, device_id={'seq': (me + p) % n}, device_id_type=pl.DeviceIdType.MESH)
        return c
    lax.fori_loop(1, n, greet, 0)

    act_ref[...] = dot(f_ref[...], we_ref[...], 1, 0).astype(BF16).astype(F32)

    def spread(r, c):
        abuf[r] = act_ref[pl.ds(r, 1), :]
        return c
    lax.fori_loop(0, n_t, spread, 0)

    def own(k, c):
        a_ref[me * tl + k] = act_ref[pl.ds(me * tl + k, 1), :]
        return c
    lax.fori_loop(0, tl, own, 0)
    pl.semaphore_wait(barrier, n - 1)

    def a_copy(p):
        to = (me + p) % n
        return pltpu.make_async_remote_copy(src_ref=abuf.at[pl.ds(to * tl, tl)], dst_ref=a_ref.at[pl.ds(me * tl, tl)], send_sem=asend.at[p],
                                            recv_sem=arecv.at[p], device_id={'seq': to}, device_id_type=pl.DeviceIdType.MESH)

    def a_go(p, c):
        a_copy(p).start()
        return c
    lax.fori_loop(1, n, a_go, 0)

    gcopy.wait()
    c_ref[...] = dot(g_ref[...], wp_ref[...], 1, 0).astype(BF16).astype(F32)
    u_row = lax.broadcasted_iota(jnp.int32, (n_u, n_u), 0)
    u_col = lax.broadcasted_iota(jnp.int32, (n_u, n_u), 1)
    lab_row = lab_ref[pl.ds(me, 1), :].astype(F32)
    lab_col = jnp.sum(jnp.where(u_row == u_col, lab_row, 0.0), axis=1, keepdims=True)
    onehot_ref[...] = jnp.where(lax.broadcasted_iota(jnp.int32, (n_u, n_v), 1).astype(F32) == lab_col, 1.0, 0.0)
    bt_ref[...] = jnp.full_like(bt_ref, NEG)
    lt_ref[...] = jnp.full_like(lt_ref, NEG)
    rs_ref[...] = jnp.zeros_like(rs_ref)

    def a_wait(p, c):
        a_copy(p).wait_recv()
        return c
    lax.fori_loop(1, n, a_wait, 0)

    lane = lax.broadcasted_iota(jnp.int32, (n_u, LANES), 1)
    u_sub = lax.broadcasted_iota(jnp.int32, (n_u, LANES), 0)

    def fwd(i, c):
        for k in range(BLK_T):
            h_ref[pl.ds((i * BLK_T + k) * n_u, n_u), :] = jnp.tanh(a_ref[i * BLK_T + k] + c_ref[...]).astype(BF16)
        z_ref[...] = dot(h_ref[pl.ds(i * rows, rows), :], wo_ref[...], 1, 0)
        for k in range(BLK_T):
            t = i * BLK_T + k
            zt = z_ref[k * n_u:(k + 1) * n_u, :]
            m = jnp.max(zt, axis=1, keepdims=True)
            e = jnp.exp(zt - m)
            s = jnp.sum(e, axis=1, keepdims=True)
            zl = jnp.sum(zt * onehot_ref[...], axis=1, keepdims=True)
            e_ref[pl.ds(t * n_u, n_u), :] = e
            lse = m + jnp.log(s)
            here = lane == t
            bt_ref[...] = jnp.where(here, zt[:, :1] - lse, bt_ref[...])
            lt_ref[...] = jnp.where(here, zl - lse, lt_ref[...])
            rs_ref[...] = jnp.where(here, 1.0 / s, rs_ref[...])
        return c
    lax.fori_loop(0, n_blk, fwd, 0)

    fill = jnp.full((LANES - n_u, LANES), NEG, F32)
    lt = jnp.where(u_sub == n_u - 1, NEG, lt_ref[...])
    sb_ref[...] = jnp.concatenate([skew(bt_ref[...], 1), fill], axis=0).T
    sl_ref[...] = jnp.concatenate([skew(lt, 1), fill], axis=0).T

    t_len = flen_ref[me]
    u_len = llen_ref[me]
    u_id = lax.broadcasted_iota(jnp.int32, (1, LANES), 1)
    bound = jnp.where(u_id == u_len, 0.0, NEG).astype(F32)
    start = jnp.where(u_id == 0, 0.0, NEG).astype(F32)
    last = n_t + n_u - 1
    al_ref[0:1, :] = start
    be_ref[last:last + 1, :] = bound
    be_ref[last + 1:last + 9, :] = jnp.full((8, LANES), NEG, F32)

    def chain(k, carry):
        alpha, beta = carry
        d = last - 1 - k
        xa = alpha + sb_ref[pl.ds(k, 1), :]
        ya = pltpu.roll(alpha + sl_ref[pl.ds(k, 1), :], 1, 1)
        xb = beta + sb_ref[pl.ds(d, 1), :]
        yb = pltpu.roll(beta, LANES - 1, 1) + sl_ref[pl.ds(d, 1), :]
        alpha = lse2(xa, ya)
        beta = jnp.where(d - u_id >= t_len, bound, lse2(xb, yb))
        al_ref[pl.ds(k + 1, 1), :] = alpha
        be_ref[pl.ds(d, 1), :] = beta
        return alpha, beta
    _, beta0 = lax.fori_loop(0, last, chain, (start, bound))
    logp = jnp.sum(jnp.where(u_id == 0, beta0, 0.0), axis=1, keepdims=True)

    d_id = lax.broadcasted_iota(jnp.int32, (LANES, LANES), 0)
    ul_id = lax.broadcasted_iota(jnp.int32, (LANES, LANES), 1)
    t_id = d_id - ul_id
    ok = (t_id >= 0) & (t_id < t_len) & (ul_id < n_u)
    up = be_ref[1:LANES + 1, :]
    base = al_ref[...] - logp
    gb = jnp.where(ok, jnp.exp(jnp.minimum(base + sb_ref[...] + up, 0.0)), 0.0)
    gl = jnp.where(ok & (ul_id < n_u - 1), jnp.exp(jnp.minimum(base + sl_ref[...] + pltpu.roll(up, LANES - 1, 1), 0.0)), 0.0)
    gb = skew(gb.T[:n_u], -1)
    gl = skew(gl.T[:n_u], -1)
    gb_ref[...] = gb
    gl_ref[...] = gl
    c1_ref[...] = (gb + gl) * rs_ref[...]

    dc_ref[...] = jnp.zeros_like(dc_ref)
    p_out[...] = jnp.zeros_like(p_out)
    v0 = lax.broadcasted_iota(jnp.int32, (n_u, LANES), 1) == 0

    def bwd(i, c):
        turn = (LANES - i * BLK_T) % LANES
        c1 = pltpu.roll(c1_ref[...], turn, 1)
        gbr = pltpu.roll(gb_ref[...], turn, 1)
        glr = pltpu.roll(gl_ref[...], turn, 1)
        for k in range(BLK_T):
            t = i * BLK_T + k
            dz = e_ref[pl.ds(t * n_u, n_u), :] * c1[:, k:k + 1] - glr[:, k:k + 1] * onehot_ref[...]
            dz_ref[k * n_u:(k + 1) * n_u, LANES:] = dz[:, LANES:].astype(BF16)
            dz_ref[k * n_u:(k + 1) * n_u, :LANES] = (dz[:, :LANES] - jnp.where(v0, gbr[:, k:k + 1], 0.0)).astype(BF16)
        hb = h_ref[pl.ds(i * rows, rows), :]
        for q in range(n_v // 256):
            r = dot(hb, dz_ref[:, q * 256:(q + 1) * 256], 0, 0)
            p_out[2 * q * n_j:(2 * q + 1) * n_j] += r[:, :LANES]
            p_out[(2 * q + 1) * n_j:(2 * q + 2) * n_j] += r[:, LANES:]
        dh = dot(dz_ref[...], wo_ref[...], 1, 1)
        hf = hb.astype(F32)
        dp = (dh * (1.0 - hf * hf)).astype(BF16).astype(F32)
        for k in range(BLK_T):
            t = i * BLK_T + k
            dpt = dp[k * n_u:(k + 1) * n_u]
            dabuf[t // tl, t % tl] = jnp.sum(dpt, axis=0, keepdims=True).astype(BF16).astype(F32)
            dc_ref[...] += dpt
        return c
    lax.fori_loop(0, n_blk, bwd, 0)

    def put_loss(s, c):
        dabuf[s, tl] = jnp.broadcast_to(-logp, (1, n_j))
        return c
    lax.fori_loop(0, n, put_loss, 0)

    def keep(k, c):
        darecv[me, k] = dabuf[me, k]
        return c
    lax.fori_loop(0, tl + 1, keep, 0)

    def d_copy(p):
        to = (me + p) % n
        return pltpu.make_async_remote_copy(src_ref=dabuf.at[to], dst_ref=darecv.at[me], send_sem=dsend.at[p],
                                            recv_sem=drecv.at[p], device_id={'seq': to}, device_id_type=pl.DeviceIdType.MESH)

    def d_go(p, c):
        d_copy(p).start()
        return c
    lax.fori_loop(1, n, d_go, 0)

    gwp = dot(g_ref[...], dc_ref[...].astype(BF16), 0, 0)
    for q in range(n_j // LANES):
        p_pred[q * n_j:(q + 1) * n_j] = gwp[:, q * LANES:(q + 1) * LANES]
    used = n_j * n_j // LANES
    if used < p_pred.shape[0]:
        p_pred[used:] = jnp.zeros((p_pred.shape[0] - used, LANES), F32)

    def d_wait(p, c):
        d_copy(p).wait_recv()
        return c
    lax.fori_loop(1, n, d_wait, 0)

    def collect(b, c):
        for k in range(tl):
            daloc[pl.ds(b * tl + k, 1), :] = darecv[b, k]
        lossbuf[pl.ds(b, 1), :] = darecv[b, tl][:, :LANES]
        return c
    lax.fori_loop(0, n, collect, 0)
    loss_ref[...] = lossbuf[...]
    dal = daloc[...].astype(BF16)
    genc_ref[...] = dot(dal, we_ref[...], 1, 1).astype(BF16)
    gwe = dot(f_ref[...], dal, 0, 0)
    n_e = f_ref.shape[1]
    for q in range(n_j // LANES):
        p_enc[q * n_e:(q + 1) * n_e] = gwe[:, q * LANES:(q + 1) * LANES]

    comm = Comm(ssem, rsem)
    pos = (core, x, y, dev)

    def six(ref, m):
        return ref.reshape(2, 2, SIDE, SIDE, m, LANES)
    ars = [AllReduce(comm, pos, six(p, p.shape[0] // 64), full, a, b, c) for p, full, a, b, c in
           ((p_out, full_out, r0o, r1o, r2o), (p_pred, full_pred, r0p, r1p, r2p), (p_enc, full_enc, r0e, r1e, r2e))]
    for step in STEPS:
        for ar in ars:
            getattr(ar, step)()

    def sends_done(p, c):
        a_copy(p).wait_send()
        d_copy(p).wait_send()
        return c
    lax.fori_loop(1, n, sends_done, 0)
    comm.drain()


def solution(mesh):
    n = mesh.shape['seq']
    assert n == 2 * SIDE * SIDE
    parts = 2 * n

    def local_fn(enc_out, pred_out, w_enc, w_pred, w_out, labels, frame_len, label_len):
        n_utt, n_loc, n_e = enc_out.shape
        _, n_u, n_g = pred_out.shape
        n_j, n_v = w_out.shape
        n_t = n_loc * n
        assert n_utt == n
        lab_ids = jnp.concatenate([labels, jnp.full((n_utt, 1), -1, jnp.int32)], axis=1)
        m_out, m_pred, m_enc = (pieces_rows(r, c, parts) for r, c in ((n_j, n_v), (n_g, n_j), (n_e, n_j)))
        vm = pl.BlockSpec(memory_space=pltpu.VMEM)
        sm = pl.BlockSpec(memory_space=pltpu.SMEM)

        def six(m):
            return (2, 2, SIDE, SIDE, m, LANES)

        def ar_scratch(m):
            return [pltpu.VMEM((2, SIDE, SIDE, m, LANES), F32), pltpu.VMEM((2, 6, 2, m, LANES), F32), pltpu.VMEM((2, 6, m, LANES), F32)]
        sq = pltpu.VMEM((LANES, LANES), F32)
        hf = pltpu.VMEM((n_u, LANES), F32)
        n_sem = 3 * 42
        outs = pl.pallas_call(
            functools.partial(kernel, n),
            out_shape=(jax.ShapeDtypeStruct((n, LANES), F32), jax.ShapeDtypeStruct((n_utt * n_loc, n_e), BF16),
                       jax.ShapeDtypeStruct(six(m_out), F32), jax.ShapeDtypeStruct(six(m_pred), F32), jax.ShapeDtypeStruct(six(m_enc), F32)),
            in_specs=[vm, pl.BlockSpec(memory_space=pl.ANY), vm, vm, vm, vm, sm, sm],
            out_specs=(vm,) * 5,
            scratch_shapes=[
                pltpu.VMEM((n_u, n_g), BF16), pltpu.VMEM((n_t, 1, n_j), F32), pltpu.VMEM((n_t, 1, n_j), F32), pltpu.VMEM((n_t, n_j), F32),
                pltpu.VMEM((n_u, n_j), F32), pltpu.VMEM((n_u, n_v), F32), pltpu.VMEM((n_t * n_u, n_j), BF16), pltpu.VMEM((BLK_T * n_u, n_v), F32),
                pltpu.VMEM((n_t * n_u, n_v), F32), hf, hf, hf,
                sq, sq, sq, pltpu.VMEM((LANES + 8, LANES), F32), hf, hf, hf, pltpu.VMEM((BLK_T * n_u, n_v), BF16), pltpu.VMEM((n_u, n_j), F32),
                pltpu.VMEM((n, n_loc + 1, 1, n_j), F32), pltpu.VMEM((n, n_loc + 1, 1, n_j), F32), pltpu.VMEM((n_t, n_j), F32), pltpu.VMEM((n, LANES), F32),
                pltpu.VMEM((parts * m_out, LANES), F32), pltpu.VMEM((parts * m_pred, LANES), F32), pltpu.VMEM((parts * m_enc, LANES), F32),
                *ar_scratch(m_out), *ar_scratch(m_pred), *ar_scratch(m_enc),
                pltpu.SemaphoreType.DMA, pltpu.SemaphoreType.DMA((n,)), pltpu.SemaphoreType.DMA((n,)), pltpu.SemaphoreType.DMA((n,)), pltpu.SemaphoreType.DMA((n,)),
                pltpu.SemaphoreType.DMA((n_sem,)), pltpu.SemaphoreType.DMA((n_sem,))],
            compiler_params=pltpu.CompilerParams(collective_id=0, has_side_effects=True, vmem_limit_bytes=62 * 1024 * 1024),
        )(enc_out.reshape(n_utt * n_loc, n_e), pred_out, w_enc, w_pred, w_out, lab_ids, frame_len, label_len)
        loss, genc, fo, fp, fe = outs

        def unflat(full, r, c):
            return full.reshape(-1, LANES)[:r * c // LANES].reshape(c // LANES, r, LANES).transpose(1, 0, 2).reshape(r, c)
        return (loss[:, 0], genc.reshape(n_utt, n_loc, n_e), unflat(fe, n_e, n_j), unflat(fp, n_g, n_j), unflat(fo, n_j, n_v))

    in_specs = (P('dp', 'seq', None), P('dp', None, None), P(None, None), P(None, None), P(None, None), P('dp', None), P('dp'), P('dp'))
    out_specs = (P('dp'), P('dp', 'seq', None), P('dp', None), P('dp', None), P('dp', None))
    return jax.shard_map(local_fn, mesh=mesh, in_specs=in_specs, out_specs=out_specs, check_vma=False)
```

```python
import functools

import jax
import jax.numpy as jnp
from jax import lax
from jax.experimental import pallas as pl
from jax.experimental.pallas import tpu as pltpu
from jax.sharding import PartitionSpec as P

NEG = -1.0e30
SIDE = 4
LANES = 128
BLK_T = 8
F32 = jnp.float32
BF16 = jnp.bfloat16


def dot(a, b, ca, cb):
    return lax.dot_general(a, b, (((ca,), (cb,)), ((), ())), preferred_element_type=F32)


def lse2(x, y):
    m = jnp.maximum(x, y)
    return m + jnp.log(1.0 + jnp.exp(-jnp.abs(x - y)))


def pieces_rows(rows, cols, parts):
    tiles = rows * cols // (8 * LANES)
    return -(-tiles // parts) * 8


class Comm:
    def __init__(self, send_sem, recv_sem):
        self.send_sem, self.recv_sem, self.used, self.sent = send_sem, recv_sem, 0, {}

    def send(self, src, dst, dev):
        k, slot = self.used, self.used % self.send_sem.shape[0]
        self.used += 1
        if slot in self.sent:
            self.sent.pop(slot).wait_send()
        cp = pltpu.make_async_remote_copy(src_ref=src, dst_ref=dst, send_sem=self.send_sem.at[slot], recv_sem=self.recv_sem.at[k],
                                          device_id={'seq': dev}, device_id_type=pl.DeviceIdType.MESH)
        cp.start()
        self.sent[slot] = cp
        return cp

    def drain(self):
        for cp in self.sent.values():
            cp.wait_send()
        self.sent = {}


class Ring:
    def __init__(self, pos, dev_of):
        self.me, self.r, self.l, self.o = pos, (pos + 1) % SIDE, (pos + 3) % SIDE, (pos + 2) % SIDE
        self.right, self.left, self.opp = dev_of(self.r), dev_of(self.l), dev_of(self.o)


def rs_start(comm, ring, view, buf):
    return (comm.send(view(ring.o, 0), buf[0], ring.right), comm.send(view(ring.o, 1), buf[2], ring.left),
            comm.send(view(ring.r, 1), buf[1], ring.right), comm.send(view(ring.l, 0), buf[3], ring.left))


def rs_mid(comm, ring, view, buf, st):
    st[0].wait_recv()
    v = view(ring.r, 0)
    v[...] += buf[0][...]
    a = comm.send(v, buf[4], ring.right)
    st[1].wait_recv()
    v = view(ring.l, 1)
    v[...] += buf[2][...]
    b = comm.send(v, buf[5], ring.left)
    return st + (a, b)


def rs_end(ring, view, buf, st, out):
    for k in (2, 3, 4, 5):
        st[k].wait_recv()
    out(0, view(ring.me, 0)[...] + buf[4][...] + buf[3][...])
    out(1, view(ring.me, 1)[...] + buf[5][...] + buf[1][...])


def ex_start(comm, ring, view, buf):
    return tuple(comm.send(view(at), b, to) for at, b, to in zip((ring.r, ring.l, ring.o), buf, (ring.right, ring.left, ring.opp)))


def ag_start(comm, ring, whole):
    v = whole(ring.me)
    return (comm.send(v, v, ring.right), comm.send(v, v, ring.left))


def ag_mid(comm, ring, half, st):
    st[0].wait_recv()
    v = half(ring.l, 0)
    a = comm.send(v, v, ring.right)
    st[1].wait_recv()
    v = half(ring.r, 1)
    b = comm.send(v, v, ring.left)
    return (a, b)


def ag_end(st):
    st[0].wait_recv()
    st[1].wait_recv()


class AllReduce:
    def __init__(self, comm, pos, full, part=None, r0=None, r1=None, r2=None):
        self.comm, (self.core, x, y, dev) = comm, pos
        self.part, self.full, self.r0, self.r1, self.r2 = part, full, r0, r1, r2
        rx = Ring(x, lambda i: dev(i, y, self.core))
        ry = Ring(y, lambda i: dev(x, i, self.core))
        self.rings = ((rx, ry), (ry, rx))
        self.sibling = dev(x, y, 1 - self.core)

    def v1(self, ref, k):
        return lambda a, half: ref.at[self.core, k, a, pl.ds(2 * half, 2)]

    def v2(self, ref, k):
        return lambda b: ref.at[self.core, k, self.rings[k][0].me, b]

    def b1(self, k):
        return [self.r1.at[k, s] for s in range(6)]

    def b2(self, k):
        return [self.r2.at[k, s] for s in range(3)]

    def d2d_start(self):
        self.st0 = self.comm.send(self.part.at[1 - self.core], self.r0, self.sibling)

    def rs1_start(self):
        self.st0.wait_recv()
        self.part[pl.ds(self.core, 1)] += self.r0[...][None]
        self.st = [rs_start(self.comm, self.rings[k][0], self.v1(self.part, k), self.b1(k)) for k in range(2)]

    def rs1_mid(self):
        self.st = [rs_mid(self.comm, self.rings[k][0], self.v1(self.part, k), self.b1(k), self.st[k]) for k in range(2)]

    def rs2_start(self):
        for k in range(2):
            view = self.v1(self.part, k)

            def put(half, val, view=view, k=k):
                view(self.rings[k][0].me, half)[...] = val
            rs_end(self.rings[k][0], view, self.b1(k), self.st[k], put)
            self.st[k] = ex_start(self.comm, self.rings[k][1], self.v2(self.part, k), self.b2(k))

    def mine(self, k):
        return self.full.at[self.core, k, self.rings[k][0].me, self.rings[k][1].me]

    def gather_start(self):
        self.st = []
        for k in range(2):
            own = self.mine(k)
            self.st.append(ex_start(self.comm, self.rings[k][1], lambda b, own=own: own, (own, own, own)))

    def ag2_start(self):
        for k in range(2):
            for cp in self.st[k]:
                cp.wait_recv()
            got = self.b2(k)
            self.mine(k)[...] = self.v2(self.part, k)(self.rings[k][1].me)[...] + got[0][...] + got[1][...] + got[2][...]
        self.gather_start()

    def ag1_start(self):
        for k in range(2):
            for cp in self.st[k]:
                cp.wait_recv()
            self.st[k] = ag_start(self.comm, self.rings[k][0], lambda a, k=k: self.full.at[self.core, k, a])

    def ag1_mid(self):
        self.st = [ag_mid(self.comm, self.rings[k][0], self.v1(self.full, k), self.st[k]) for k in range(2)]

    def d2d_back(self):
        for k in range(2):
            ag_end(self.st[k])
        half = self.full.at[self.core]
        self.st0 = self.comm.send(half, half, self.sibling)

    def finish(self):
        self.st0.wait_recv()


def skew(mat):
    return pltpu.roll(mat, 0, 1, stride=1, stride_axis=0)


def unskew(mat):
    rows = lax.broadcasted_iota(jnp.int32, mat.shape, 0)
    bit = 1
    while bit < mat.shape[0]:
        mat = jnp.where((rows & bit) != 0, pltpu.roll(mat, LANES - bit, 1), mat)
        bit *= 2
    return mat


def lse(terms):
    m = functools.reduce(jnp.maximum, terms)
    return m + jnp.log(functools.reduce(jnp.add, [jnp.exp(x - m) for x in terms]))


def shift(x, k):
    return x if k == 0 else pltpu.roll(x, k % LANES, 1)


def compose(first, second):
    r = len(first) - 1
    return [lse([shift(first[k - j], j) + second[j] for j in range(max(0, k - r), min(r, k) + 1)]) for k in range(2 * r + 1)]


def every(ref, k, start, step):
    return ref[k, pl.ds(start, LANES // step, stride=step), :]


def lattice(w_refs, al_ref, be_ref, start, bound, levels):
    for lv in range(levels):
        src, dst, rows = w_refs[lv], w_refs[lv + 1], LANES >> lv
        r = 2 ** lv
        first = [src[k, pl.ds(0, rows // 2, stride=2), :] for k in range(r + 1)]
        second = [src[k, pl.ds(1, rows // 2, stride=2), :] for k in range(r + 1)]
        for k, w in enumerate(compose(first, second)):
            dst[k, :rows // 2, :] = w
    hop = 2 ** levels
    top, n_hop = w_refs[levels], LANES // hop
    al_ref[0:1, :] = start
    be_ref[LANES:LANES + 8, :] = jnp.broadcast_to(bound, (8, LANES))

    def chain(i, carry):
        alpha, beta = carry
        j = n_hop - 1 - i
        alpha = lse([shift(alpha, k) + top[k, pl.ds(i, 1), :] for k in range(hop + 1)])
        beta = lse([shift(beta + top[k, pl.ds(j, 1), :], -k) for k in range(hop + 1)])
        al_ref[pl.ds((i + 1) * hop, 1), :] = alpha
        be_ref[pl.ds(j * hop, 1), :] = beta
        return alpha, beta
    lax.fori_loop(0, n_hop, chain, (start, bound))
    for lv in range(levels - 1, -1, -1):
        r = 2 ** lv
        n_r = LANES // (2 * r)
        al = al_ref[pl.ds(0, n_r, stride=2 * r), :]
        be = be_ref[pl.ds(2 * r, n_r, stride=2 * r), :]
        al_ref[pl.ds(r, n_r, stride=2 * r), :] = lse([shift(al, k) + w_refs[lv][k, pl.ds(0, n_r, stride=2), :] for k in range(r + 1)])
        be_ref[pl.ds(r, n_r, stride=2 * r), :] = lse([shift(be + w_refs[lv][k, pl.ds(1, n_r, stride=2), :], -k) for k in range(r + 1)])


LEVELS = 3


def kernel(n, f_hbm, pred_ref, we_hbm, wp_hbm, wo_hbm, lab_ref, flen_ref, llen_ref,
           loss_out, genc_out, gwe_out, gwp_out, gwo_out,
           f_ref, we_ref, wp_ref, wo_ref, g_ref, abuf, a_ref, act_ref, c_ref, onehot_ref, h_ref, z0_ref, z1_ref, e_ref, bt_ref, lt_ref, rs_ref,
           w0, w1, w2, w3, al_ref, be_ref, c1_ref, gb_ref, gl_ref, dz0_ref, dz1_ref, dc_ref, dabuf, darecv, daloc, loss_col, lossbuf, genc_ref,
           fg_ref, dg_ref, p_out, p_pred, s_out, s_pred, r0a, r1a, r2a, r0b, r1b, r2b, r0p, r1p, r2p,
           insem, outsem, asend, arecv, dsend, drecv, ssem, rsem):
    me = lax.axis_index('seq')
    core, x, y = me % 2, (me // 2) % SIDE, me // (2 * SIDE)

    def dev(i, j, c):
        return (j * SIDE + i) * 2 + c

    n_t, n_u, n_j, n_v = n * a_ref.shape[1], c_ref.shape[0], c_ref.shape[1], wo_ref.shape[1]
    n_e = f_ref.shape[2]
    tl = n_t // n
    rows = BLK_T * n_u
    n_blk = n_t // BLK_T
    n_h = n_v // 2

    barrier = pltpu.get_barrier_semaphore()

    def greet(p, c):
        pl.semaphore_signal(barrier, inc=1, device_id={'seq': (me + p) % n}, device_id_type=pl.DeviceIdType.MESH)
        return c
    lax.fori_loop(1, n, greet, 0)
    loads = [pltpu.make_async_copy(src, dst, insem.at[k]) for k, (src, dst) in enumerate(
        ((f_hbm, f_ref), (we_hbm, we_ref), (pred_ref.at[me], g_ref), (wp_hbm, wp_ref), (wo_hbm, wo_ref)))]
    for cp in loads:
        cp.start()
    comm = Comm(ssem, rsem)
    pos = (core, x, y, dev)

    def six(ref, base, m):
        return ref.at[pl.ds(base, 64 * m)].reshape(2, 2, SIDE, SIDE, m, LANES)
    m_o, m_p = n_j * n_h // LANES // 64, p_pred.shape[0] // 64
    ar0 = AllReduce(comm, pos, six(s_out, 0, m_o), six(p_out, 0, m_o), r0a, r1a, r2a)
    ar1 = AllReduce(comm, pos, six(s_out, 64 * m_o, m_o), six(p_out, 64 * m_o, m_o), r0b, r1b, r2b)
    arp = AllReduce(comm, pos, six(s_pred, 0, m_p), six(p_pred, 0, m_p), r0p, r1p, r2p)
    agf = AllReduce(comm, pos, fg_ref)
    agd = AllReduce(comm, pos, dg_ref)

    loads[0].wait()
    loads[1].wait()
    for k in range(tl):
        agf.mine(k)[...] = f_ref[:, k, :]
    f_loc = jnp.concatenate([agf.mine(k)[...] for k in range(tl)], axis=0)
    act_ref[...] = dot(f_loc, we_ref[...], 1, 0).astype(BF16).astype(F32)

    def spread(b, c):
        for k in range(tl):
            abuf[b, k] = act_ref[pl.ds(k * n + b, 1), :]
        return c
    lax.fori_loop(0, n, spread, 0)
    for k in range(tl):
        a_ref[me, k] = act_ref[pl.ds(k * n + me, 1), :]
    pl.semaphore_wait(barrier, n - 1)

    def a_copy(p):
        to = (me + p) % n
        return pltpu.make_async_remote_copy(src_ref=abuf.at[to], dst_ref=a_ref.at[me], send_sem=asend, recv_sem=arecv, device_id={'seq': to}, device_id_type=pl.DeviceIdType.MESH)

    def a_go(p, c):
        a_copy(p).start()
        return c
    lax.fori_loop(1, n, a_go, 0)
    agf.gather_start()

    loads[2].wait()
    loads[3].wait()
    c_ref[...] = dot(g_ref[...], wp_ref[...], 1, 0).astype(BF16).astype(F32)
    n_lab = lab_ref.shape[1]
    u_row = lax.broadcasted_iota(jnp.int32, (n_u, n_lab), 0)
    u_col = lax.broadcasted_iota(jnp.int32, (n_u, n_lab), 1)
    lab_row = lab_ref[pl.ds(me, 1), :].astype(F32)
    lab_col = jnp.sum(jnp.where(u_row == u_col, lab_row, 0.0), axis=1, keepdims=True)
    lab_col = jnp.where(lax.broadcasted_iota(jnp.int32, (n_u, 1), 0) < n_lab, lab_col, -1.0)
    onehot_ref[...] = jnp.where(lax.broadcasted_iota(jnp.int32, (n_u, n_v), 1).astype(F32) == lab_col, 1.0, 0.0)
    bt_ref[...] = jnp.full_like(bt_ref, NEG)
    lt_ref[...] = jnp.full_like(lt_ref, NEG)
    rs_ref[...] = jnp.zeros_like(rs_ref)
    loads[4].wait()

    others = pl.ds(0, n - 1)
    pltpu.make_async_copy(abuf.at[others], a_ref.at[others], arecv).wait()

    lane = lax.broadcasted_iota(jnp.int32, (n_u, LANES), 1)
    u_sub = lax.broadcasted_iota(jnp.int32, (n_u, LANES), 0)

    def scores(i, z_ref):
        for k in range(BLK_T):
            h_ref[pl.ds((i * BLK_T + k) * n_u, n_u), :] = jnp.tanh(a_ref[(i * BLK_T + k) // tl, (i * BLK_T + k) % tl] + c_ref[...]).astype(BF16)
        z_ref[...] = dot(h_ref[pl.ds(i * rows, rows), :], wo_ref[...], 1, 0)

    def stats(i, z_ref):
        for k in range(BLK_T):
            t = i * BLK_T + k
            zt = z_ref[k * n_u:(k + 1) * n_u, :]
            m = jnp.max(zt, axis=1, keepdims=True)
            e = jnp.exp(zt - m)
            s = jnp.sum(e, axis=1, keepdims=True)
            zl = jnp.sum(zt * onehot_ref[...], axis=1, keepdims=True)
            e_ref[pl.ds(t * n_u, n_u), :] = e
            norm = m + jnp.log(s)
            here = lane == t
            bt_ref[...] = jnp.where(here, zt[:, :1] - norm, bt_ref[...])
            lt_ref[...] = jnp.where(here, zl - norm, lt_ref[...])
            rs_ref[...] = jnp.where(here, 1.0 / s, rs_ref[...])

    def pair(i, c):
        scores(2 * i + 1, z1_ref)
        stats(2 * i, z0_ref)
        scores(2 * i + 2, z0_ref)
        stats(2 * i + 1, z1_ref)
        return c
    scores(0, z0_ref)
    n_pair = n_blk // 2 - 1
    lax.fori_loop(0, 1, pair, 0)
    agf.ag1_start()
    lax.fori_loop(1, n_pair, pair, 0)
    scores(n_blk - 1, z1_ref)
    stats(n_blk - 2, z0_ref)
    stats(n_blk - 1, z1_ref)
    agf.ag1_mid()

    t_len = flen_ref[me]
    u_len = llen_ref[me]
    fill = jnp.full((LANES - n_u, LANES), NEG, F32)
    lt = jnp.where(u_sub == n_u - 1, NEG, lt_ref[...])
    d_id = lax.broadcasted_iota(jnp.int32, (LANES, LANES), 0)
    u_id = lax.broadcasted_iota(jnp.int32, (LANES, LANES), 1)
    t_id = d_id - u_id
    past = t_id >= t_len
    sb = jnp.concatenate([skew(bt_ref[...]), fill], axis=0).T
    sl = jnp.concatenate([skew(lt), fill], axis=0).T
    sb = jnp.where(past, jnp.where(u_id == u_len, 0.0, NEG), jnp.where(t_id < 0, NEG, sb))
    sl = jnp.where(past | (t_id < 0), NEG, sl)
    w0[0] = sb
    w0[1] = pltpu.roll(sl, 1, 1)
    row_id = lax.broadcasted_iota(jnp.int32, (1, LANES), 1)
    bound = jnp.where(row_id == u_len, 0.0, NEG).astype(F32)
    start = jnp.where(row_id == 0, 0.0, NEG).astype(F32)
    lattice((w0, w1, w2, w3), al_ref, be_ref, start, bound, LEVELS)
    logp = jnp.sum(jnp.where(row_id == 0, be_ref[0:1, :], 0.0), axis=1, keepdims=True)
    ok = (t_id >= 0) & jnp.logical_not(past) & (u_id < n_u)
    up = be_ref[1:LANES + 1, :]
    base = al_ref[:LANES, :] - logp
    gb = jnp.where(ok, jnp.exp(jnp.minimum(base + w0[0] + up, 0.0)), 0.0)
    gl = jnp.where(ok & (u_id < n_u - 1), jnp.exp(jnp.minimum(base + pltpu.roll(w0[1] + up, LANES - 1, 1), 0.0)), 0.0)
    gb = unskew(gb.T[:n_u])
    gl = unskew(gl.T[:n_u])
    gb_ref[...] = gb
    gl_ref[...] = gl
    c1_ref[...] = (gb + gl) * rs_ref[...]

    for b in range(n):
        dabuf[b, tl] = jnp.broadcast_to(-logp, (1, n_j))
    dc_ref[...] = jnp.zeros_like(dc_ref)
    p_out[...] = jnp.zeros_like(p_out)
    v0 = lax.broadcasted_iota(jnp.int32, (n_u, LANES), 1) == 0

    def grad_logits(i, lo, dz_ref):
        turn = (LANES - i * BLK_T) % LANES
        c1 = pltpu.roll(c1_ref[...], turn, 1)
        gbr = pltpu.roll(gb_ref[...], turn, 1)
        glr = pltpu.roll(gl_ref[...], turn, 1)
        for k in range(BLK_T):
            at = (i * BLK_T + k) * n_u
            dz = e_ref[pl.ds(at, n_u), lo:lo + n_h] * c1[:, k:k + 1] - glr[:, k:k + 1] * onehot_ref[:, lo:lo + n_h]
            if lo == 0:
                dz_ref[pl.ds(at, n_u), LANES:] = dz[:, LANES:].astype(BF16)
                dz_ref[pl.ds(at, n_u), :LANES] = (dz[:, :LANES] - jnp.where(v0, gbr[:, k:k + 1], 0.0)).astype(BF16)
            else:
                dz_ref[pl.ds(at, n_u), :] = dz.astype(BF16)

    def grad_out(i, q0, dz_ref):
        hb = h_ref[pl.ds(i * 2 * rows, 2 * rows), :]
        r = dot(hb, dz_ref[pl.ds(i * 2 * rows, 2 * rows), :], 0, 0)
        for q in range(n_h // LANES):
            p_out[(q0 + q) * n_j:(q0 + q + 1) * n_j] += r[:, q * LANES:(q + 1) * LANES]

    def phase0(i, c):
        grad_logits(i, 0, dz0_ref)
        return c

    def phase1(i, c):
        grad_out(i, 0, dz0_ref)
        grad_logits(2 * i, n_h, dz1_ref)
        grad_logits(2 * i + 1, n_h, dz1_ref)
        return c

    def phase2(i, c):
        grad_out(i, n_h // LANES, dz1_ref)
        return c

    def grad_hidden(i, z_ref):
        at = pl.ds(i * rows, rows)
        z_ref[:, :n_j] = dot(dz0_ref[at, :], wo_ref[:, :n_h], 1, 1) + dot(dz1_ref[at, :], wo_ref[:, n_h:], 1, 1)

    def grad_pre(i, z_ref):
        for k in range(BLK_T):
            t = i * BLK_T + k
            hf = h_ref[pl.ds(t * n_u, n_u), :].astype(F32)
            dpt = (z_ref[k * n_u:(k + 1) * n_u, :n_j] * (1.0 - hf * hf)).astype(BF16).astype(F32)
            dabuf[t // tl, t % tl] = jnp.sum(dpt, axis=0, keepdims=True).astype(BF16).astype(F32)
            dc_ref[...] += dpt

    def phase3(i, c):
        grad_hidden(2 * i + 1, z1_ref)
        grad_pre(2 * i, z0_ref)
        grad_hidden(2 * i + 2, z0_ref)
        grad_pre(2 * i + 1, z1_ref)
        return c

    lax.fori_loop(0, n_blk, phase0, 0)
    agf.d2d_back()
    lax.fori_loop(0, n_blk // 2, phase1, 0)
    ar0.d2d_start()
    lax.fori_loop(0, n_blk // 4, phase2, 0)
    ar0.rs1_start()
    lax.fori_loop(n_blk // 4, n_blk // 2, phase2, 0)
    ar1.d2d_start()
    grad_hidden(0, z0_ref)
    lax.fori_loop(0, 1, phase3, 0)
    ar1.rs1_start()
    ar0.rs1_mid()
    lax.fori_loop(1, 2, phase3, 0)
    ar1.rs1_mid()
    lax.fori_loop(2, n_pair, phase3, 0)
    ar0.rs2_start()
    grad_hidden(n_blk - 1, z1_ref)
    grad_pre(n_blk - 2, z0_ref)
    grad_pre(n_blk - 1, z1_ref)

    def keep(k, c):
        darecv[me, k] = dabuf[me, k]
        return c
    lax.fori_loop(0, tl + 1, keep, 0)

    def d_copy(p):
        to = (me + p) % n
        return pltpu.make_async_remote_copy(src_ref=dabuf.at[to], dst_ref=darecv.at[me], send_sem=dsend, recv_sem=drecv, device_id={'seq': to}, device_id_type=pl.DeviceIdType.MESH)

    def d_go(p, c):
        d_copy(p).start()
        return c
    lax.fori_loop(1, n, d_go, 0)

    gwp = dot(g_ref[...], dc_ref[...].astype(BF16), 0, 0)
    for q in range(n_j // LANES):
        p_pred[q * n_j:(q + 1) * n_j] = gwp[:, q * LANES:(q + 1) * LANES]
    used = n_j * n_j // LANES
    if used < p_pred.shape[0]:
        p_pred[used:] = jnp.zeros((p_pred.shape[0] - used, LANES), F32)
    arp.d2d_start()
    ar1.rs2_start()
    ar0.ag2_start()
    arp.rs1_start()
    ar1.ag2_start()
    pltpu.make_async_copy(dabuf.at[others], darecv.at[others], drecv).wait()

    def collect(b, c):
        for k in range(tl):
            daloc[pl.ds(k * n + b, 1), :] = darecv[b, k]
        loss_col[pl.ds(b, 1), :] = darecv[b, tl][:, :n]
        return c
    lax.fori_loop(0, n, collect, 0)
    dal = daloc[...].astype(BF16)
    for k in range(2):
        agd.mine(k)[...] = dal[k * n:(k + 1) * n, :]
    agd.gather_start()
    ar0.ag1_start()
    arp.rs1_mid()
    diag = lax.broadcasted_iota(jnp.int32, (n, n), 0) == lax.broadcasted_iota(jnp.int32, (n, n), 1)
    lossbuf[...] = jnp.sum(jnp.where(diag, loss_col[...], 0.0), axis=0, keepdims=True)
    genc = dot(dal, we_ref[...], 1, 1).astype(BF16)
    for k in range(tl):
        genc_ref[:, k, :] = genc[k * n:(k + 1) * n, :]
    flush = []

    def put(src, dst):
        cp = pltpu.make_async_copy(src, dst, outsem.at[len(flush)])
        cp.start()
        flush.append(cp)
    put(lossbuf, loss_out)
    put(genc_ref, genc_out)
    agd.ag1_start()
    ar0.ag1_mid()
    ar1.ag1_start()
    arp.rs2_start()
    agd.ag1_mid()
    ar1.ag1_mid()
    arp.ag2_start()
    ar0.d2d_back()
    agd.d2d_back()
    ar1.d2d_back()
    arp.ag1_start()
    agf.finish()
    agd.finish()

    at_o, at_e, at_p = 0, n_j, n_j + n_e
    blk = n_e // 4

    def enc_block(i, c):
        fb = fg_ref[:, :, :, :, :, pl.ds(pl.multiple_of(i * blk, blk), blk)].reshape(n * n_t, blk)
        e_ref[pl.ds(pl.multiple_of(at_e + i * blk, 8), blk), :n_j] = dot(fb, dg_ref[...].reshape(n * n_t, n_j), 0, 0)
        return c
    lax.fori_loop(0, 4, enc_block, 0)
    put(e_ref.at[pl.ds(at_e, n_e), pl.ds(0, n_j)], gwe_out)
    arp.ag1_mid()
    ar0.finish()
    for q in range(n_h // LANES):
        e_ref[at_o:at_o + n_j, q * LANES:(q + 1) * LANES] = s_out[q * n_j:(q + 1) * n_j]
    put(e_ref.at[pl.ds(at_o, n_j), pl.ds(0, n_h)], gwo_out.at[:, pl.ds(0, n_h)])
    ar1.finish()
    for q in range(n_h // LANES, n_v // LANES):
        e_ref[at_o:at_o + n_j, q * LANES:(q + 1) * LANES] = s_out[q * n_j:(q + 1) * n_j]
    put(e_ref.at[pl.ds(at_o, n_j), pl.ds(n_h, n_h)], gwo_out.at[:, pl.ds(n_h, n_h)])
    arp.d2d_back()
    arp.finish()
    n_g = g_ref.shape[1]
    for q in range(n_j // LANES):
        e_ref[at_p:at_p + n_g, q * LANES:(q + 1) * LANES] = s_pred[q * n_g:(q + 1) * n_g]
    put(e_ref.at[pl.ds(at_p, n_g), pl.ds(0, n_j)], gwp_out)

    pltpu.make_async_copy(abuf.at[others], a_ref.at[others], asend).wait()
    pltpu.make_async_copy(dabuf.at[others], darecv.at[others], dsend).wait()
    comm.drain()
    for cp in flush:
        cp.wait()


def move(*refs):
    half = len(refs) // 2
    for src, dst in zip(refs[:half], refs[half:]):
        dst[...] = src[...]


def solution(mesh):
    n = mesh.shape['seq']
    assert n == 2 * SIDE * SIDE
    parts = 2 * n

    def local_fn(enc_out, pred_out, w_enc, w_pred, w_out, labels, frame_len, label_len):
        n_utt, n_loc, n_e = enc_out.shape
        _, n_u, n_g = pred_out.shape
        n_j, n_v = w_out.shape
        n_t = n_loc * n
        assert n_utt == n
        m_o, m_p = pieces_rows(n_j, n_v // 2, parts), pieces_rows(n_g, n_j, parts)
        vm = pl.BlockSpec(memory_space=pltpu.VMEM)
        sm = pl.BlockSpec(memory_space=pltpu.SMEM)
        hbm = pl.BlockSpec(memory_space=pl.ANY)

        def ar_scratch(m):
            return [pltpu.VMEM((2, SIDE, SIDE, m, LANES), F32), pltpu.VMEM((2, 6, 2, m, LANES), F32), pltpu.VMEM((2, 3, m, LANES), F32)]
        hf = pltpu.VMEM((n_u, LANES), F32)
        n_sem = 3 * 34 + 2 * 15
        row = pltpu.VMEM((n, n_loc, 1, n_j), F32)
        msg = pltpu.VMEM((n, n_loc + 1, 1, n_j), F32)
        levels = [pltpu.VMEM((2 ** lv + 1, LANES >> lv, LANES), F32) for lv in range(LEVELS + 1)]
        shapes = tuple(jax.ShapeDtypeStruct(*a) for a in (((1, n), F32), ((n_utt, n_loc, n_e), BF16), ((n_e, n_j), F32), ((n_g, n_j), F32), ((n_j, n_v), F32)))
        outs = pl.pallas_call(
            functools.partial(kernel, n),
            out_shape=shapes,
            in_specs=[hbm, hbm, hbm, hbm, hbm, vm, sm, sm],
            out_specs=(hbm,) * 5,
            scratch_shapes=[
                pltpu.VMEM((n_utt, n_loc, n_e), BF16), pltpu.VMEM((n_e, n_j), BF16), pltpu.VMEM((n_g, n_j), BF16), pltpu.VMEM((n_j, n_v), BF16),
                pltpu.VMEM((n_u, n_g), BF16), row, row, pltpu.VMEM((n_t, n_j), F32),
                pltpu.VMEM((n_u, n_j), F32), pltpu.VMEM((n_u, n_v), F32), pltpu.VMEM((n_t * n_u, n_j), BF16),
                pltpu.VMEM((BLK_T * n_u, n_v), F32), pltpu.VMEM((BLK_T * n_u, n_v), F32),
                pltpu.VMEM((n_t * n_u, n_v), F32), hf, hf, hf,
                *levels, pltpu.VMEM((LANES + 8, LANES), F32), pltpu.VMEM((LANES + 8, LANES), F32), hf, hf, hf,
                pltpu.VMEM((n_t * n_u, n_v // 2), BF16), pltpu.VMEM((n_t * n_u, n_v // 2), BF16), pltpu.VMEM((n_u, n_j), F32),
                msg, msg, pltpu.VMEM((n_t, n_j), F32), pltpu.VMEM((n, n), F32), pltpu.VMEM((1, n), F32), pltpu.VMEM((n_utt, n_loc, n_e), BF16),
                pltpu.VMEM((2, 2, SIDE, SIDE, n, n_e), BF16), pltpu.VMEM((2, 2, SIDE, SIDE, n, n_j), BF16),
                pltpu.VMEM((2 * parts * m_o, LANES), F32), pltpu.VMEM((parts * m_p, LANES), F32),
                pltpu.VMEM((2 * parts * m_o, LANES), F32), pltpu.VMEM((parts * m_p, LANES), F32),
                *ar_scratch(m_o), *ar_scratch(m_o), *ar_scratch(m_p),
                pltpu.SemaphoreType.DMA((5,)), pltpu.SemaphoreType.DMA((6,)),
                pltpu.SemaphoreType.DMA, pltpu.SemaphoreType.DMA, pltpu.SemaphoreType.DMA, pltpu.SemaphoreType.DMA,
                pltpu.SemaphoreType.DMA((32,)), pltpu.SemaphoreType.DMA((n_sem,))],
            compiler_params=pltpu.CompilerParams(collective_id=0, has_side_effects=True, vmem_limit_bytes=63 * 1024 * 1024),
        )(enc_out, pred_out, w_enc, w_pred, w_out, labels, frame_len, label_len)
        steps = 8
        specs = tuple(pl.BlockSpec((o.shape[0] // steps,) + o.shape[1:], lambda i, d=len(o.shape): (i,) + (0,) * (d - 1)) if o.shape[0] > 1 else
                      pl.BlockSpec(o.shape, lambda i: (0, 0)) for o in shapes)
        loss, genc, gwe, gwp, gwo = pl.pallas_call(move, grid=(steps,), out_shape=shapes, in_specs=list(specs), out_specs=specs)(*outs)
        return loss.reshape(n), genc, gwe, gwp, gwo

    in_specs = (P('dp', 'seq', None), P('dp', None, None), P(None, None), P(None, None), P(None, None), P('dp', None), P('dp'), P('dp'))
    out_specs = (P('dp'), P('dp', 'seq', None), P('dp', None), P('dp', None), P('dp', None))
    return jax.shard_map(local_fn, mesh=mesh, in_specs=in_specs, out_specs=out_specs, check_vma=False)
```

```python
import functools

import jax
import jax.numpy as jnp
from jax import lax
from jax.experimental import pallas as pl
from jax.experimental.pallas import tpu as pltpu
from jax.sharding import PartitionSpec as P

NEG = -1.0e30
SIDE = 4
LANES = 128
BLK_T = 8
F32 = jnp.float32
BF16 = jnp.bfloat16


def dot(a, b, ca, cb):
    return lax.dot_general(a, b, (((ca,), (cb,)), ((), ())), preferred_element_type=F32)


def lse2(x, y):
    m = jnp.maximum(x, y)
    return m + jnp.log(1.0 + jnp.exp(-jnp.abs(x - y)))


def pieces_rows(rows, cols, parts):
    tiles = rows * cols // (8 * LANES)
    return -(-tiles // parts) * 8


class Comm:
    def __init__(self, send_sem, recv_sem):
        self.send_sem, self.recv_sem, self.used, self.sent = send_sem, recv_sem, 0, {}

    def send(self, src, dst, dev):
        k, slot = self.used, self.used % self.send_sem.shape[0]
        self.used += 1
        if slot in self.sent:
            self.sent.pop(slot).wait_send()
        cp = pltpu.make_async_remote_copy(src_ref=src, dst_ref=dst, send_sem=self.send_sem.at[slot], recv_sem=self.recv_sem.at[k],
                                          device_id={'seq': dev}, device_id_type=pl.DeviceIdType.MESH)
        cp.start()
        self.sent[slot] = cp
        return cp

    def drain(self):
        for cp in self.sent.values():
            cp.wait_send()
        self.sent = {}


class Ring:
    def __init__(self, pos, dev_of):
        self.me, self.r, self.l, self.o = pos, (pos + 1) % SIDE, (pos + 3) % SIDE, (pos + 2) % SIDE
        self.right, self.left, self.opp = dev_of(self.r), dev_of(self.l), dev_of(self.o)


def rs_start(comm, ring, view, buf):
    return (comm.send(view(ring.o, 0), buf[0], ring.right), comm.send(view(ring.o, 1), buf[2], ring.left),
            comm.send(view(ring.r, 1), buf[1], ring.right), comm.send(view(ring.l, 0), buf[3], ring.left))


def rs_mid(comm, ring, view, buf, st):
    st[0].wait_recv()
    v = view(ring.r, 0)
    v[...] += buf[0][...]
    a = comm.send(v, buf[4], ring.right)
    st[1].wait_recv()
    v = view(ring.l, 1)
    v[...] += buf[2][...]
    b = comm.send(v, buf[5], ring.left)
    return st + (a, b)


def rs_end(ring, view, buf, st, out):
    for k in (2, 3, 4, 5):
        st[k].wait_recv()
    out(0, view(ring.me, 0)[...] + buf[4][...] + buf[3][...])
    out(1, view(ring.me, 1)[...] + buf[5][...] + buf[1][...])


def ex_start(comm, ring, view, buf):
    return tuple(comm.send(view(at), b, to) for at, b, to in zip((ring.r, ring.l, ring.o), buf, (ring.right, ring.left, ring.opp)))


def ag_start(comm, ring, whole):
    v = whole(ring.me)
    return (comm.send(v, v, ring.right), comm.send(v, v, ring.left))


def ag_mid(comm, ring, half, st):
    st[0].wait_recv()
    v = half(ring.l, 0)
    a = comm.send(v, v, ring.right)
    st[1].wait_recv()
    v = half(ring.r, 1)
    b = comm.send(v, v, ring.left)
    return (a, b)


def ag_end(st):
    st[0].wait_recv()
    st[1].wait_recv()


class AllReduce:
    def __init__(self, comm, pos, full, part=None, r0=None, r1=None, r2=None, relay=False):
        self.comm, (self.core, x, y, dev) = comm, pos
        self.part, self.full, self.r0, self.r1, self.r2, self.relay = part, full, r0, r1, r2, relay
        rx = Ring(x, lambda i: dev(i, y, self.core))
        ry = Ring(y, lambda i: dev(x, i, self.core))
        self.rings = ((rx, ry), (ry, rx))
        self.sibling = dev(x, y, 1 - self.core)
        n = full.shape[4]
        self.spans = ((0, n // 32 * 16), (n // 32 * 16, n - n // 32 * 16))

    def v1(self, ref, k):
        return lambda a, half: ref.at[self.core, k, a, pl.ds(2 * half, 2)]

    def v2(self, ref, k):
        return lambda b: ref.at[self.core, k, self.rings[k][0].me, b]

    def v2h(self, ref, k):
        return lambda b, half: ref.at[self.core, k, self.rings[k][0].me, b, pl.ds(*self.spans[half])]

    def b1(self, k):
        return [self.r1.at[k, s] for s in range(6)]

    def b2(self, k):
        return [self.r2.at[k, s] for s in range(3)]

    def b2h(self, k):
        return [self.r2.at[k, s, pl.ds(*self.spans[half])] for s, half in enumerate((0, 1, 1, 0, 0, 1))]

    def mine(self, k):
        return self.full.at[self.core, k, self.rings[k][0].me, self.rings[k][1].me]

    def d2d_start(self):
        self.st0 = self.comm.send(self.part.at[1 - self.core], self.r0, self.sibling)

    def rs1_start(self):
        if self.r0 is not None:
            self.st0.wait_recv()
            self.part[pl.ds(self.core, 1)] += self.r0[...][None]
        self.st = [rs_start(self.comm, self.rings[k][0], self.v1(self.part, k), self.b1(k)) for k in range(2)]

    def rs1_mid(self):
        self.st = [rs_mid(self.comm, self.rings[k][0], self.v1(self.part, k), self.b1(k), self.st[k]) for k in range(2)]

    def rs2_start(self):
        for k in range(2):
            view = self.v1(self.part, k)

            def put(half, val, view=view, k=k):
                view(self.rings[k][0].me, half)[...] = val
            rs_end(self.rings[k][0], view, self.b1(k), self.st[k], put)
            if self.relay:
                self.st[k] = rs_start(self.comm, self.rings[k][1], self.v2h(self.part, k), self.b2h(k))
            else:
                self.st[k] = ex_start(self.comm, self.rings[k][1], self.v2(self.part, k), self.b2(k))

    def rs2_mid(self):
        self.st = [rs_mid(self.comm, self.rings[k][1], self.v2h(self.part, k), self.b2h(k), self.st[k]) for k in range(2)]

    def ag2_start(self):
        for k in range(2):
            if self.relay:
                dst = self.v2h(self.full, k)

                def put(half, val, dst=dst, k=k):
                    dst(self.rings[k][1].me, half)[...] = val
                rs_end(self.rings[k][1], self.v2h(self.part, k), self.b2h(k), self.st[k], put)
            else:
                for cp in self.st[k]:
                    cp.wait_recv()
                got = self.b2(k)
                self.mine(k)[...] = self.v2(self.part, k)(self.rings[k][1].me)[...] + got[0][...] + got[1][...] + got[2][...]
        self.gather_start()

    def gather_start(self):
        self.st = []
        for k in range(2):
            own, ring = self.mine(k), self.rings[k][1]
            if self.relay:
                self.st.append((self.comm.send(own, own, ring.right), self.comm.send(own, own, ring.left)))
            else:
                self.st.append(ex_start(self.comm, ring, lambda b, own=own: own, (own, own, own)))

    def ag2_mid(self):
        self.st = [ag_mid(self.comm, self.rings[k][1], self.v2h(self.full, k), self.st[k]) for k in range(2)]

    def ag1_start(self):
        for k in range(2):
            for cp in self.st[k]:
                cp.wait_recv()
            self.st[k] = ag_start(self.comm, self.rings[k][0], lambda a, k=k: self.full.at[self.core, k, a])

    def ag1_mid(self):
        self.st = [ag_mid(self.comm, self.rings[k][0], self.v1(self.full, k), self.st[k]) for k in range(2)]

    def d2d_back(self):
        for k in range(2):
            ag_end(self.st[k])
        half = self.full.at[self.core]
        self.st0 = self.comm.send(half, half, self.sibling)

    def finish(self):
        self.st0.wait_recv()


def skew(mat):
    return pltpu.roll(mat, 0, 1, stride=1, stride_axis=0)


def unskew(mat):
    rows = lax.broadcasted_iota(jnp.int32, mat.shape, 0)
    bit = 1
    while bit < mat.shape[0]:
        mat = jnp.where((rows & bit) != 0, pltpu.roll(mat, LANES - bit, 1), mat)
        bit *= 2
    return mat


def lse(terms):
    m = functools.reduce(jnp.maximum, terms)
    return m + jnp.log(functools.reduce(jnp.add, [jnp.exp(x - m) for x in terms]))


def shift(x, k):
    return x if k == 0 else pltpu.roll(x, k % LANES, 1)


def compose(first, second):
    r = len(first) - 1
    return [lse([shift(first[k - j], j) + second[j] for j in range(max(0, k - r), min(r, k) + 1)]) for k in range(2 * r + 1)]


def every(ref, k, start, step):
    return ref[k, pl.ds(start, LANES // step, stride=step), :]


def lattice(w_refs, al_ref, be_ref, start, bound, levels):
    for lv in range(levels):
        src, dst, rows = w_refs[lv], w_refs[lv + 1], LANES >> lv
        r = 2 ** lv
        first = [src[k, pl.ds(0, rows // 2, stride=2), :] for k in range(r + 1)]
        second = [src[k, pl.ds(1, rows // 2, stride=2), :] for k in range(r + 1)]
        for k, w in enumerate(compose(first, second)):
            dst[k, :rows // 2, :] = w
    hop = 2 ** levels
    top, n_hop = w_refs[levels], LANES // hop
    al_ref[0:1, :] = start
    be_ref[LANES:LANES + 8, :] = jnp.broadcast_to(bound, (8, LANES))

    def chain(i, carry):
        alpha, beta = carry
        j = n_hop - 1 - i
        alpha = lse([shift(alpha, k) + top[k, pl.ds(i, 1), :] for k in range(hop + 1)])
        beta = lse([shift(beta + top[k, pl.ds(j, 1), :], -k) for k in range(hop + 1)])
        al_ref[pl.ds((i + 1) * hop, 1), :] = alpha
        be_ref[pl.ds(j * hop, 1), :] = beta
        return alpha, beta
    lax.fori_loop(0, n_hop, chain, (start, bound))
    for lv in range(levels - 1, -1, -1):
        r = 2 ** lv
        n_r = LANES // (2 * r)
        al = al_ref[pl.ds(0, n_r, stride=2 * r), :]
        be = be_ref[pl.ds(2 * r, n_r, stride=2 * r), :]
        al_ref[pl.ds(r, n_r, stride=2 * r), :] = lse([shift(al, k) + w_refs[lv][k, pl.ds(0, n_r, stride=2), :] for k in range(r + 1)])
        be_ref[pl.ds(r, n_r, stride=2 * r), :] = lse([shift(be + w_refs[lv][k, pl.ds(1, n_r, stride=2), :], -k) for k in range(r + 1)])


LEVELS = 3
BLK_G = 2


def kernel(n, f_hbm, pred_ref, we_hbm, wp_hbm, wo_hbm, lab_ref, flen_ref, llen_ref,
           loss_out, genc_out, gwe_out, gwp_out, gwo_out,
           f_ref, we_ref, wp_ref, wo_ref, g_ref, abuf, a_ref, act_ref, c_ref, onehot_ref, h_ref, z0_ref, z1_ref, e_ref, bt_ref, lt_ref, rs_ref,
           w0, w1, w2, w3, al_ref, be_ref, c1_ref, gb_ref, gl_ref, dz_ref, dc_ref, dabuf, darecv,
           fg_ref, dg_ref, p_out, p_pred, r0a, r1a, r2a, r1p, r2p,
           insem, asend, arecv, dsend, drecv, ssem, rsem):
    me = lax.axis_index('seq')
    core, x, y = me % 2, (me // 2) % SIDE, me // (2 * SIDE)

    def dev(i, j, c):
        return (j * SIDE + i) * 2 + c

    n_t, n_u, n_j, n_v = n * a_ref.shape[1], c_ref.shape[0], c_ref.shape[1], wo_ref.shape[1]
    n_e = f_ref.shape[2]
    tl = n_t // n
    rows = BLK_T * n_u
    n_blk = n_t // BLK_T

    barrier = pltpu.get_barrier_semaphore()

    loads = [pltpu.make_async_copy(src, dst, insem.at[k]) for k, (src, dst) in enumerate(
        ((f_hbm, f_ref), (we_hbm, we_ref), (pred_ref.at[pl.ds(me - core, 2)], g_ref), (wp_hbm, wp_ref), (wo_hbm, wo_ref)))]
    for cp in loads:
        cp.start()
    def greet(p, c):
        pl.semaphore_signal(barrier, inc=1, device_id={'seq': (me + p) % n}, device_id_type=pl.DeviceIdType.MESH)
        return c
    lax.fori_loop(1, n, greet, 0)
    comm = Comm(ssem, rsem)
    pos = (core, x, y, dev)

    def six(ref, base, m):
        return ref.at[pl.ds(base, 64 * m)].reshape(2, 2, SIDE, SIDE, m, LANES)
    m_o, m_p = n_j * n_v // LANES // 64, p_pred.shape[0] // 64
    at_p = 64 * m_o
    aro = AllReduce(comm, pos, six(e_ref, 0, m_o), six(p_out, 0, m_o), r0a, r1a, r2a, relay=True)
    arp = AllReduce(comm, pos, six(e_ref, at_p, m_p), six(p_pred, 0, m_p), None, r1p, r2p)
    agf = AllReduce(comm, pos, fg_ref)
    agd = AllReduce(comm, pos, dg_ref)

    loads[0].wait()
    loads[1].wait()
    for k in range(tl):
        agf.mine(k)[...] = f_ref[:, k, :]
    f_loc = jnp.concatenate([agf.mine(k)[...] for k in range(tl)], axis=0)
    act_ref[...] = dot(f_loc, we_ref[...], 1, 0).astype(BF16).astype(F32)

    def spread(b, c):
        for k in range(tl):
            abuf[b, k] = act_ref[pl.ds(k * n + b, 1), :]
        return c
    lax.fori_loop(0, n, spread, 0)
    for k in range(tl):
        a_ref[me, k] = act_ref[pl.ds(k * n + me, 1), :]
    pl.semaphore_wait(barrier, n - 1)

    def a_copy(p):
        to = (me + p) % n
        return pltpu.make_async_remote_copy(src_ref=abuf.at[to], dst_ref=a_ref.at[me], send_sem=asend, recv_sem=arecv, device_id={'seq': to}, device_id_type=pl.DeviceIdType.MESH)

    def a_go(p, c):
        a_copy(p).start()
        return c
    lax.fori_loop(1, n, a_go, 0)
    agf.gather_start()

    loads[2].wait()
    loads[3].wait()
    c_ref[...] = dot(g_ref[core], wp_ref[...], 1, 0).astype(BF16).astype(F32)
    n_lab = lab_ref.shape[1]
    u_row = lax.broadcasted_iota(jnp.int32, (n_u, n_lab), 0)
    u_col = lax.broadcasted_iota(jnp.int32, (n_u, n_lab), 1)
    lab_row = lab_ref[pl.ds(me, 1), :].astype(F32)
    lab_col = jnp.sum(jnp.where(u_row == u_col, lab_row, 0.0), axis=1, keepdims=True)
    lab_col = jnp.where(lax.broadcasted_iota(jnp.int32, (n_u, 1), 0) < n_lab, lab_col, -1.0)
    onehot_ref[...] = jnp.where(lax.broadcasted_iota(jnp.int32, (n_u, n_v), 1).astype(F32) == lab_col, 1.0, 0.0)
    bt_ref[...] = jnp.full_like(bt_ref, NEG)
    lt_ref[...] = jnp.full_like(lt_ref, NEG)
    rs_ref[...] = jnp.zeros_like(rs_ref)
    loads[4].wait()

    others = pl.ds(0, n - 1)
    pltpu.make_async_copy(abuf.at[others], a_ref.at[others], arecv).wait()

    lane = lax.broadcasted_iota(jnp.int32, (n_u, LANES), 1)
    u_sub = lax.broadcasted_iota(jnp.int32, (n_u, LANES), 0)

    def scores(i, z_ref):
        for k in range(BLK_T):
            h_ref[pl.ds((i * BLK_T + k) * n_u, n_u), :] = jnp.tanh(a_ref[(i * BLK_T + k) // tl, (i * BLK_T + k) % tl] + c_ref[...]).astype(BF16)
        z_ref[...] = dot(h_ref[pl.ds(i * rows, rows), :], wo_ref[...], 1, 0)

    def stats(i, z_ref):
        for k in range(BLK_T):
            t = i * BLK_T + k
            zt = z_ref[k * n_u:(k + 1) * n_u, :]
            m = jnp.max(zt, axis=1, keepdims=True)
            e = jnp.exp(zt - m)
            s = jnp.sum(e, axis=1, keepdims=True)
            zl = jnp.sum(zt * onehot_ref[...], axis=1, keepdims=True)
            for q in range(n_v // LANES):
                e_ref[pl.ds(q * n_t * n_u + t * n_u, n_u), :] = e[:, q * LANES:(q + 1) * LANES]
            norm = m + jnp.log(s)
            here = lane == t
            bt_ref[...] = jnp.where(here, zt[:, :1] - norm, bt_ref[...])
            lt_ref[...] = jnp.where(here, zl - norm, lt_ref[...])
            rs_ref[...] = jnp.where(here, 1.0 / s, rs_ref[...])

    def pair(i, c):
        scores(2 * i + 1, z1_ref)
        stats(2 * i, z0_ref)
        scores(2 * i + 2, z0_ref)
        stats(2 * i + 1, z1_ref)
        return c
    scores(0, z0_ref)
    n_pair = n_blk // 2 - 1
    lax.fori_loop(0, 1, pair, 0)
    agf.ag1_start()
    lax.fori_loop(1, n_pair, pair, 0)
    scores(n_blk - 1, z1_ref)
    stats(n_blk - 2, z0_ref)
    stats(n_blk - 1, z1_ref)

    t_len = flen_ref[me]
    u_len = llen_ref[me]
    fill = jnp.full((LANES - n_u, LANES), NEG, F32)
    lt = jnp.where(u_sub == n_u - 1, NEG, lt_ref[...])
    d_id = lax.broadcasted_iota(jnp.int32, (LANES, LANES), 0)
    u_id = lax.broadcasted_iota(jnp.int32, (LANES, LANES), 1)
    t_id = d_id - u_id
    past = t_id >= t_len
    sb = jnp.concatenate([skew(bt_ref[...]), fill], axis=0).T
    sl = jnp.concatenate([skew(lt), fill], axis=0).T
    sb = jnp.where(past, jnp.where(u_id == u_len, 0.0, NEG), jnp.where(t_id < 0, NEG, sb))
    sl = jnp.where(past | (t_id < 0), NEG, sl)
    w0[0] = sb
    w0[1] = pltpu.roll(sl, 1, 1)
    row_id = lax.broadcasted_iota(jnp.int32, (1, LANES), 1)
    bound = jnp.where(row_id == u_len, 0.0, NEG).astype(F32)
    start = jnp.where(row_id == 0, 0.0, NEG).astype(F32)
    lattice((w0, w1, w2, w3), al_ref, be_ref, start, bound, LEVELS)
    logp = jnp.sum(jnp.where(row_id == 0, be_ref[0:1, :], 0.0), axis=1, keepdims=True)
    ok = (t_id >= 0) & jnp.logical_not(past) & (u_id < n_u)
    up = be_ref[1:LANES + 1, :]
    base = al_ref[:LANES, :] - logp
    gb = jnp.where(ok, jnp.exp(jnp.minimum(base + w0[0] + up, 0.0)), 0.0)
    gl = jnp.where(ok & (u_id < n_u - 1), jnp.exp(jnp.minimum(base + pltpu.roll(w0[1] + up, LANES - 1, 1), 0.0)), 0.0)
    gb = unskew(gb.T[:n_u])
    gl = unskew(gl.T[:n_u])
    gb_ref[...] = gb
    gl_ref[...] = gl
    c1_ref[...] = (gb + gl) * rs_ref[...]

    dc_ref[core] = jnp.zeros(dc_ref.shape[1:], F32)
    dc_ref[core, n_u:n_u + 1, :] = jnp.broadcast_to(-logp, (1, n_j))
    v0 = lax.broadcasted_iota(jnp.int32, (n_u, LANES), 1) == 0

    def grad_logits(i):
        turn = (LANES - i * BLK_T) % LANES
        c1 = pltpu.roll(c1_ref[...], turn, 1)
        gbr = pltpu.roll(gb_ref[...], turn, 1)
        glr = pltpu.roll(gl_ref[...], turn, 1)
        for k in range(BLK_T):
            at = (i * BLK_T + k) * n_u
            for q in range(n_v // LANES):
                cols = slice(q * LANES, (q + 1) * LANES)
                dz = e_ref[q * n_t * n_u + at:q * n_t * n_u + at + n_u, :] * c1[:, k:k + 1] - glr[:, k:k + 1] * onehot_ref[:, cols]
                if q == 0:
                    dz = dz - jnp.where(v0, gbr[:, k:k + 1], 0.0)
                dz_ref[at:at + n_u, cols] = dz.astype(BF16)

    def grad_out(i):
        at = slice(i * BLK_G * rows, (i + 1) * BLK_G * rows)
        r = dot(h_ref[at, :], dz_ref[at, :], 0, 0)
        for q in range(n_v // LANES):
            part = r[:, q * LANES:(q + 1) * LANES]
            p_out[q * n_j:(q + 1) * n_j] = part if i == 0 else p_out[q * n_j:(q + 1) * n_j] + part

    def grad_hidden(i, z_ref):
        z_ref[:, :n_j] = dot(dz_ref[pl.ds(i * rows, rows), :], wo_ref[...], 1, 1)

    def grad_pre(i, z_ref):
        row = []
        for k in range(BLK_T):
            t = i * BLK_T + k
            hf = h_ref[pl.ds(t * n_u, n_u), :].astype(F32)
            dpt = (z_ref[k * n_u:(k + 1) * n_u, :n_j] * (1.0 - hf * hf)).astype(BF16).astype(F32)
            row.append(jnp.sum(dpt, axis=0, keepdims=True))
            if len(row) == tl:
                dabuf[t // tl] = jnp.concatenate(row, axis=0).astype(BF16)
                row = []
            dc_ref[core, :n_u, :] += dpt

    def phase3(i, c):
        grad_hidden(2 * i + 1, z1_ref)
        grad_pre(2 * i, z0_ref)
        grad_hidden(2 * i + 2, z0_ref)
        grad_pre(2 * i + 1, z1_ref)
        return c

    for k in range(BLK_G):
        grad_logits(k)
    agf.ag1_mid()
    for i in range(n_blk // BLK_G):
        grad_out(i)
        if i + 1 < n_blk // BLK_G:
            for k in range(BLK_G):
                grad_logits(BLK_G * (i + 1) + k)
    aro.d2d_start()
    grad_hidden(0, z0_ref)
    lax.fori_loop(0, 1, phase3, 0)
    aro.rs1_start()
    agf.d2d_back()
    lax.fori_loop(1, n_pair, phase3, 0)
    grad_hidden(n_blk - 1, z1_ref)
    grad_pre(n_blk - 2, z0_ref)
    grad_pre(n_blk - 1, z1_ref)

    own_dc = dc_ref.at[core]
    dc_copy = comm.send(own_dc, own_dc, aro.sibling)
    darecv[me] = dabuf[me]
    aro.rs1_mid()

    def d_copy(p):
        to = (me + p) % n
        return pltpu.make_async_remote_copy(src_ref=dabuf.at[to], dst_ref=darecv.at[me], send_sem=dsend, recv_sem=drecv, device_id={'seq': to}, device_id_type=pl.DeviceIdType.MESH)

    def d_go(p, c):
        d_copy(p).start()
        return c
    lax.fori_loop(1, n, d_go, 0)

    dc_copy.wait_recv()
    n_g = g_ref.shape[2]
    gwp = dot(g_ref[...].reshape(2 * n_u, n_g), dc_ref[:, :n_u, :].reshape(2 * n_u, n_j).astype(BF16), 0, 0)
    for q in range(n_j // LANES):
        p_pred[q * n_g:(q + 1) * n_g] = gwp[:, q * LANES:(q + 1) * LANES]
    used = n_g * n_j // LANES
    spare = lax.broadcasted_iota(jnp.int32, (p_pred.shape[0] - used, LANES), 0) - me + core
    p_pred[used:] = jnp.where(spare == 0, dc_ref[0, n_u:n_u + 1, :LANES], jnp.where(spare == 1, dc_ref[1, n_u:n_u + 1, :LANES], 0.0))
    arp.rs1_start()
    aro.rs2_start()
    pltpu.make_async_copy(dabuf.at[others], darecv.at[others], drecv).wait()

    dal = jnp.concatenate([darecv[:, k, :] for k in range(tl)], axis=0)
    for k in range(2):
        agd.mine(k)[...] = dal[k * n:(k + 1) * n, :]
    agd.gather_start()
    aro.rs2_mid()
    genc = dot(dal, we_ref[...], 1, 1).astype(BF16)
    for k in range(tl):
        genc_out[:, k, :] = genc[k * n:(k + 1) * n, :]
    arp.rs1_mid()
    agd.ag1_start()
    aro.ag2_start()
    arp.rs2_start()
    aro.ag2_mid()
    agd.ag1_mid()
    arp.ag2_start()
    aro.ag1_start()
    agd.d2d_back()

    blk = n_e // 4

    def enc_block(i, side, first):
        fb = fg_ref[side, :, :, :, :, pl.ds(pl.multiple_of(i * blk, blk), blk)].reshape(n * n_t // 2, blk)
        r = dot(fb, dg_ref[side].reshape(n * n_t // 2, n_j), 0, 0)
        at = pl.ds(pl.multiple_of(i * blk, blk), blk)
        gwe_out[at, :] = r if first else gwe_out[at, :] + r

    def enc_own(i, c):
        enc_block(i, core, True)
        return c

    def enc_other(i, c):
        enc_block(i, 1 - core, False)
        return c

    def put_cols(base, n_r, dst):
        for q in range(dst.shape[1] // LANES):
            dst[:, q * LANES:(q + 1) * LANES] = e_ref[base + q * n_r:base + (q + 1) * n_r]
    lax.fori_loop(0, 4, enc_own, 0)
    arp.ag1_start()
    aro.ag1_mid()
    agf.finish()
    agd.finish()
    lax.fori_loop(0, 4, enc_other, 0)
    arp.ag1_mid()
    aro.d2d_back()
    arp.d2d_back()
    aro.finish()
    put_cols(0, n_j, gwo_out)
    arp.finish()
    put_cols(at_p, n_g, gwp_out)
    diag = lax.broadcasted_iota(jnp.int32, (n, n), 0) == lax.broadcasted_iota(jnp.int32, (n, n), 1)
    loss_out[...] = jnp.sum(jnp.where(diag, e_ref[at_p + used:at_p + used + n, :n], 0.0), axis=0, keepdims=True)
    pltpu.make_async_copy(abuf.at[others], a_ref.at[others], asend).wait()
    pltpu.make_async_copy(dabuf.at[others], darecv.at[others], dsend).wait()
    comm.drain()


def move(count, *refs):
    src, dst, sem = refs[:count], refs[count:2 * count], refs[2 * count]
    copies = [pltpu.make_async_copy(a, b, sem.at[k]) for k, (a, b) in enumerate(zip(src, dst))]
    for cp in copies:
        cp.start()
    for cp in copies:
        cp.wait()


def solution(mesh):
    n = mesh.shape['seq']
    assert n == 2 * SIDE * SIDE
    parts = 2 * n

    def local_fn(enc_out, pred_out, w_enc, w_pred, w_out, labels, frame_len, label_len):
        n_utt, n_loc, n_e = enc_out.shape
        _, n_u, n_g = pred_out.shape
        n_j, n_v = w_out.shape
        n_t = n_loc * n
        assert n_utt == n
        m_o, m_p = pieces_rows(n_j, n_v, parts), pieces_rows(n_g, n_j, parts)
        assert parts * m_p >= n_g * n_j // LANES + n
        vm = pl.BlockSpec(memory_space=pltpu.VMEM)
        sm = pl.BlockSpec(memory_space=pltpu.SMEM)
        hbm = pl.BlockSpec(memory_space=pl.ANY)

        def ar_scratch(m):
            return [pltpu.VMEM((2, 6, 2, m, LANES), F32), pltpu.VMEM((2, 6, m, LANES), F32)]
        hf = pltpu.VMEM((n_u, LANES), F32)
        n_sem = 42 + 33 + 2 * 15 + 1
        row = pltpu.VMEM((n, n_loc, 1, n_j), F32)
        msg = pltpu.VMEM((n, n_loc, n_j), BF16)
        levels = [pltpu.VMEM((2 ** lv + 1, LANES >> lv, LANES), F32) for lv in range(LEVELS + 1)]
        shapes = tuple(jax.ShapeDtypeStruct(*a) for a in (((1, n), F32), ((n_utt, n_loc, n_e), BF16), ((n_e, n_j), F32), ((n_g, n_j), F32), ((n_j, n_v), F32)))
        outs = pl.pallas_call(
            functools.partial(kernel, n),
            out_shape=tuple(pltpu.VMEM(o.shape, o.dtype) for o in shapes),
            in_specs=[hbm, hbm, hbm, hbm, hbm, vm, sm, sm],
            out_specs=(vm,) * 5,
            scratch_shapes=[
                pltpu.VMEM((n_utt, n_loc, n_e), BF16), pltpu.VMEM((n_e, n_j), BF16), pltpu.VMEM((n_g, n_j), BF16), pltpu.VMEM((n_j, n_v), BF16),
                pltpu.VMEM((2, n_u, n_g), BF16), row, row, pltpu.VMEM((n_t, n_j), F32),
                pltpu.VMEM((n_u, n_j), F32), pltpu.VMEM((n_u, n_v), F32), pltpu.VMEM((n_t * n_u, n_j), BF16),
                pltpu.VMEM((BLK_T * n_u, n_v), F32), pltpu.VMEM((BLK_T * n_u, n_v), F32),
                pltpu.VMEM((n_t * n_u * n_v // LANES, LANES), F32), hf, hf, hf,
                *levels, pltpu.VMEM((LANES + 8, LANES), F32), pltpu.VMEM((LANES + 8, LANES), F32), hf, hf, hf,
                pltpu.VMEM((n_t * n_u, n_v), BF16), pltpu.VMEM((2, n_u + 8, n_j), F32),
                msg, msg,
                pltpu.VMEM((2, 2, SIDE, SIDE, n, n_e), BF16), pltpu.VMEM((2, 2, SIDE, SIDE, n, n_j), BF16),
                pltpu.VMEM((parts * m_o, LANES), F32), pltpu.VMEM((parts * m_p, LANES), F32),
                pltpu.VMEM((2, SIDE, SIDE, m_o, LANES), F32), *ar_scratch(m_o), *ar_scratch(m_p),
                pltpu.SemaphoreType.DMA((5,)),
                pltpu.SemaphoreType.DMA, pltpu.SemaphoreType.DMA, pltpu.SemaphoreType.DMA, pltpu.SemaphoreType.DMA,
                pltpu.SemaphoreType.DMA((48,)), pltpu.SemaphoreType.DMA((n_sem,))],
            compiler_params=pltpu.CompilerParams(collective_id=0, has_side_effects=True, vmem_limit_bytes=57 * 1024 * 1024 - 128 * 1024),
        )(enc_out, pred_out, w_enc, w_pred, w_out, labels, frame_len, label_len)
        loss, genc, gwe, gwp, gwo = pl.pallas_call(
            functools.partial(move, len(shapes)), out_shape=shapes, in_specs=[vm] * len(shapes), out_specs=(hbm,) * len(shapes),
            scratch_shapes=[pltpu.SemaphoreType.DMA((len(shapes),))], compiler_params=pltpu.CompilerParams(vmem_limit_bytes=256 * 1024))(*outs)
        return loss.reshape(n), genc, gwe, gwp, gwo

    in_specs = (P('dp', 'seq', None), P('dp', None, None), P(None, None), P(None, None), P(None, None), P('dp', None), P('dp'), P('dp'))
    out_specs = (P('dp'), P('dp', 'seq', None), P('dp', None), P('dp', None), P('dp', None))
    return jax.shard_map(local_fn, mesh=mesh, in_specs=in_specs, out_specs=out_specs, check_vma=False)
```

```python
import functools

import jax
import jax.numpy as jnp
from jax import lax
from jax.experimental import pallas as pl
from jax.experimental.pallas import tpu as pltpu
from jax.sharding import PartitionSpec as P

NEG = -1.0e30
SIDE = 4
LANES = 128
BLK_T = 8
F32 = jnp.float32
BF16 = jnp.bfloat16


def dot(a, b, ca, cb):
    return lax.dot_general(a, b, (((ca,), (cb,)), ((), ())), preferred_element_type=F32)


def lse2(x, y):
    m = jnp.maximum(x, y)
    return m + jnp.log(1.0 + jnp.exp(-jnp.abs(x - y)))


def pieces_rows(rows, cols, parts):
    tiles = rows * cols // (8 * LANES)
    return -(-tiles // parts) * 8


class Comm:
    def __init__(self, send_sem, recv_sem):
        self.send_sem, self.recv_sem, self.used, self.sent = send_sem, recv_sem, 0, {}

    def send(self, src, dst, dev):
        k, slot = self.used, self.used % self.send_sem.shape[0]
        self.used += 1
        if slot in self.sent:
            self.sent.pop(slot).wait_send()
        cp = pltpu.make_async_remote_copy(src_ref=src, dst_ref=dst, send_sem=self.send_sem.at[slot], recv_sem=self.recv_sem.at[k],
                                          device_id={'seq': dev}, device_id_type=pl.DeviceIdType.MESH)
        cp.start()
        self.sent[slot] = cp
        return cp

    def drain(self):
        for cp in self.sent.values():
            cp.wait_send()
        self.sent = {}


class Ring:
    def __init__(self, pos, dev_of):
        self.me, self.r, self.l, self.o = pos, (pos + 1) % SIDE, (pos + 3) % SIDE, (pos + 2) % SIDE
        self.right, self.left, self.opp = dev_of(self.r), dev_of(self.l), dev_of(self.o)


def rs_start(comm, ring, view, buf):
    return (comm.send(view(ring.o, 0), buf[0], ring.right), comm.send(view(ring.o, 1), buf[2], ring.left),
            comm.send(view(ring.r, 1), buf[1], ring.right), comm.send(view(ring.l, 0), buf[3], ring.left))


def rs_mid(comm, ring, view, buf, st):
    st[0].wait_recv()
    v = view(ring.r, 0)
    v[...] += buf[0][...]
    a = comm.send(v, buf[4], ring.right)
    st[1].wait_recv()
    v = view(ring.l, 1)
    v[...] += buf[2][...]
    b = comm.send(v, buf[5], ring.left)
    return st + (a, b)


def rs_end(ring, view, buf, st, out):
    for k in (2, 3, 4, 5):
        st[k].wait_recv()
    out(0, view(ring.me, 0)[...] + buf[4][...] + buf[3][...])
    out(1, view(ring.me, 1)[...] + buf[5][...] + buf[1][...])


def ex_start(comm, ring, view, buf):
    return tuple(comm.send(view(at), b, to) for at, b, to in zip((ring.r, ring.l, ring.o), buf, (ring.right, ring.left, ring.opp)))


def ag_start(comm, ring, whole):
    v = whole(ring.me)
    return (comm.send(v, v, ring.right), comm.send(v, v, ring.left))


def ag_mid(comm, ring, half, st):
    st[0].wait_recv()
    v = half(ring.l, 0)
    a = comm.send(v, v, ring.right)
    st[1].wait_recv()
    v = half(ring.r, 1)
    b = comm.send(v, v, ring.left)
    return (a, b)


def ag_end(st):
    st[0].wait_recv()
    st[1].wait_recv()


class AllReduce:
    def __init__(self, comm, pos, full, part=None, r0=None, r1=None, r2=None, relay=False):
        self.comm, (self.core, x, y, dev) = comm, pos
        self.part, self.full, self.r0, self.r1, self.r2, self.relay = part, full, r0, r1, r2, relay
        rx = Ring(x, lambda i: dev(i, y, self.core))
        ry = Ring(y, lambda i: dev(x, i, self.core))
        self.rings = ((rx, ry), (ry, rx))
        self.sibling = dev(x, y, 1 - self.core)
        n = full.shape[4]
        self.spans = ((0, n // 32 * 16), (n // 32 * 16, n - n // 32 * 16))

    def v1(self, ref, k):
        return lambda a, half: ref.at[self.core, k, a, pl.ds(2 * half, 2)]

    def v2(self, ref, k):
        return lambda b: ref.at[self.core, k, self.rings[k][0].me, b]

    def v2h(self, ref, k):
        return lambda b, half: ref.at[self.core, k, self.rings[k][0].me, b, pl.ds(*self.spans[half])]

    def b1(self, k):
        return [self.r1.at[k, s] for s in range(6)]

    def b2(self, k):
        return [self.r2.at[k, s] for s in range(3)]

    def b2h(self, k):
        return [self.r2.at[k, s, pl.ds(*self.spans[half])] for s, half in enumerate((0, 1, 1, 0, 0, 1))]

    def mine(self, k):
        return self.full.at[self.core, k, self.rings[k][0].me, self.rings[k][1].me]

    def d2d_start(self):
        self.st0 = self.comm.send(self.part.at[1 - self.core], self.r0, self.sibling)

    def rs1_start(self):
        if self.r0 is not None:
            self.st0.wait_recv()
            self.part[pl.ds(self.core, 1)] += self.r0[...][None]
        self.st = [rs_start(self.comm, self.rings[k][0], self.v1(self.part, k), self.b1(k)) for k in range(2)]

    def rs1_mid(self):
        self.st = [rs_mid(self.comm, self.rings[k][0], self.v1(self.part, k), self.b1(k), self.st[k]) for k in range(2)]

    def rs2_start(self):
        for k in range(2):
            view = self.v1(self.part, k)

            def put(half, val, view=view, k=k):
                view(self.rings[k][0].me, half)[...] = val
            rs_end(self.rings[k][0], view, self.b1(k), self.st[k], put)
            if self.relay:
                self.st[k] = rs_start(self.comm, self.rings[k][1], self.v2h(self.part, k), self.b2h(k))
            else:
                self.st[k] = ex_start(self.comm, self.rings[k][1], self.v2(self.part, k), self.b2(k))

    def rs2_mid(self):
        self.st = [rs_mid(self.comm, self.rings[k][1], self.v2h(self.part, k), self.b2h(k), self.st[k]) for k in range(2)]

    def ag2_start(self):
        for k in range(2):
            if self.relay:
                dst = self.v2h(self.full, k)

                def put(half, val, dst=dst, k=k):
                    dst(self.rings[k][1].me, half)[...] = val
                rs_end(self.rings[k][1], self.v2h(self.part, k), self.b2h(k), self.st[k], put)
            else:
                for cp in self.st[k]:
                    cp.wait_recv()
                got = self.b2(k)
                self.mine(k)[...] = self.v2(self.part, k)(self.rings[k][1].me)[...] + got[0][...] + got[1][...] + got[2][...]
        self.gather_start()

    def gather_start(self):
        self.st = []
        for k in range(2):
            own, ring = self.mine(k), self.rings[k][1]
            if self.relay:
                self.st.append((self.comm.send(own, own, ring.right), self.comm.send(own, own, ring.left)))
            else:
                self.st.append(ex_start(self.comm, ring, lambda b, own=own: own, (own, own, own)))

    def ag2_mid(self):
        self.st = [ag_mid(self.comm, self.rings[k][1], self.v2h(self.full, k), self.st[k]) for k in range(2)]

    def ag1_start(self):
        for k in range(2):
            for cp in self.st[k]:
                cp.wait_recv()
            self.st[k] = ag_start(self.comm, self.rings[k][0], lambda a, k=k: self.full.at[self.core, k, a])

    def ag1_mid(self):
        self.st = [ag_mid(self.comm, self.rings[k][0], self.v1(self.full, k), self.st[k]) for k in range(2)]

    def d2d_back(self):
        for k in range(2):
            ag_end(self.st[k])
        half = self.full.at[self.core]
        self.st0 = self.comm.send(half, half, self.sibling)

    def finish(self):
        self.st0.wait_recv()


def skew(mat):
    return pltpu.roll(mat, 0, 1, stride=1, stride_axis=0)


def unskew(mat):
    rows = lax.broadcasted_iota(jnp.int32, mat.shape, 0)
    bit = 1
    while bit < mat.shape[0]:
        mat = jnp.where((rows & bit) != 0, pltpu.roll(mat, LANES - bit, 1), mat)
        bit *= 2
    return mat


def lse(terms):
    m = functools.reduce(jnp.maximum, terms)
    return m + jnp.log(functools.reduce(jnp.add, [jnp.exp(x - m) for x in terms]))


def shift(x, k):
    return x if k == 0 else pltpu.roll(x, k % LANES, 1)


def compose(first, second):
    r = len(first) - 1
    return [lse([shift(first[k - j], j) + second[j] for j in range(max(0, k - r), min(r, k) + 1)]) for k in range(2 * r + 1)]


def every(ref, k, start, step):
    return ref[k, pl.ds(start, LANES // step, stride=step), :]


def lattice(w_refs, al_ref, be_ref, start, bound, levels):
    for lv in range(levels):
        src, dst, rows = w_refs[lv], w_refs[lv + 1], LANES >> lv
        r = 2 ** lv
        first = [src[k, pl.ds(0, rows // 2, stride=2), :] for k in range(r + 1)]
        second = [src[k, pl.ds(1, rows // 2, stride=2), :] for k in range(r + 1)]
        for k, w in enumerate(compose(first, second)):
            dst[k, :rows // 2, :] = w
    hop = 2 ** levels
    top, n_hop = w_refs[levels], LANES // hop
    al_ref[0:1, :] = start
    be_ref[LANES:LANES + 8, :] = jnp.broadcast_to(bound, (8, LANES))

    def chain(i, carry):
        alpha, beta = carry
        j = n_hop - 1 - i
        alpha = lse([shift(alpha, k) + top[k, pl.ds(i, 1), :] for k in range(hop + 1)])
        beta = lse([shift(beta + top[k, pl.ds(j, 1), :], -k) for k in range(hop + 1)])
        al_ref[pl.ds((i + 1) * hop, 1), :] = alpha
        be_ref[pl.ds(j * hop, 1), :] = beta
        return alpha, beta
    lax.fori_loop(0, n_hop, chain, (start, bound))
    for lv in range(levels - 1, -1, -1):
        r = 2 ** lv
        n_r = LANES // (2 * r)
        al = al_ref[pl.ds(0, n_r, stride=2 * r), :]
        be = be_ref[pl.ds(2 * r, n_r, stride=2 * r), :]
        al_ref[pl.ds(r, n_r, stride=2 * r), :] = lse([shift(al, k) + w_refs[lv][k, pl.ds(0, n_r, stride=2), :] for k in range(r + 1)])
        be_ref[pl.ds(r, n_r, stride=2 * r), :] = lse([shift(be + w_refs[lv][k, pl.ds(1, n_r, stride=2), :], -k) for k in range(r + 1)])


LEVELS = 3
BLK_G = 2


def kernel(n, f_hbm, pred_ref, we_hbm, wp_hbm, wo_hbm, lab_ref, flen_ref, llen_ref,
           loss_out, genc_out, gwe_out, gwp_out, gwo_out,
           f_ref, we_ref, wp_ref, wo_ref, g_ref, abuf, arecv_buf, a_ref, c_ref, onehot_ref, h_ref, z0_ref, z1_ref, e_ref, bt_ref, lt_ref, rs_ref,
           w0, w1, w2, w3, al_ref, be_ref, c1_ref, gb_ref, gl_ref, dz_ref, dc_ref, dabuf, darecv,
           fg_ref, dg_ref, p_out, r0a, r1a, r2a, r1p, r2p,
           insem, asend, arecv, dsend, drecv, ssem, rsem):
    me = lax.axis_index('seq')
    core, x, y = me % 2, (me // 2) % SIDE, me // (2 * SIDE)

    def dev(i, j, c):
        return (j * SIDE + i) * 2 + c

    n_t, n_u, n_j, n_v = n * a_ref.shape[1], c_ref.shape[0], c_ref.shape[1], wo_ref.shape[1]
    n_e = f_ref.shape[2]
    tl = n_t // n
    rows = BLK_T * n_u
    n_blk = n_t // BLK_T

    barrier = pltpu.get_barrier_semaphore()

    loads = [pltpu.make_async_copy(src, dst, insem.at[k]) for k, (src, dst) in enumerate(
        ((f_hbm, f_ref), (we_hbm, we_ref), (pred_ref.at[pl.ds(me - core, 2)], g_ref), (wp_hbm, wp_ref), (wo_hbm, wo_ref)))]
    for cp in loads:
        cp.start()
    def greet(p, c):
        pl.semaphore_signal(barrier, inc=1, device_id={'seq': (me + p) % n}, device_id_type=pl.DeviceIdType.MESH)
        return c
    lax.fori_loop(1, n, greet, 0)
    comm = Comm(ssem, rsem)
    pos = (core, x, y, dev)

    def six(ref, base, m):
        return ref.at[pl.ds(base, 64 * m)].reshape(2, 2, SIDE, SIDE, m, LANES)
    m_o = n_j * n_v // LANES // 64
    m_p = r2p.shape[2]
    at_p = 64 * m_o
    p_pred = e_ref.at[pl.ds(at_p + 64 * m_p, 64 * m_p)]
    aro = AllReduce(comm, pos, six(e_ref, 0, m_o), six(p_out, 0, m_o), r0a, r1a, r2a, relay=True)
    arp = AllReduce(comm, pos, six(e_ref, at_p, m_p), six(e_ref, at_p + 64 * m_p, m_p), None, r1p, r2p)
    agf = AllReduce(comm, pos, fg_ref)
    agd = AllReduce(comm, pos, dg_ref, relay=True)

    loads[0].wait()
    loads[1].wait()
    for k in range(tl):
        agf.mine(k)[...] = f_ref[:, k, :]
    f_loc = jnp.concatenate([agf.mine(k)[...] for k in range(tl)], axis=0)
    act = dot(f_loc, we_ref[...], 1, 0).astype(BF16)
    for k in range(tl):
        abuf[:, k, :] = act[k * n:(k + 1) * n, :]
    arecv_buf[me] = abuf[me]
    pl.semaphore_wait(barrier, n - 1)

    def a_copy(p):
        to = (me + p) % n
        return pltpu.make_async_remote_copy(src_ref=abuf.at[to], dst_ref=arecv_buf.at[me], send_sem=asend, recv_sem=arecv, device_id={'seq': to}, device_id_type=pl.DeviceIdType.MESH)

    def a_go(p, c):
        a_copy(p).start()
        return c
    lax.fori_loop(1, n, a_go, 0)
    agf.gather_start()

    loads[2].wait()
    loads[3].wait()
    c_ref[...] = dot(g_ref[core], wp_ref[...], 1, 0).astype(BF16).astype(F32)
    n_lab = lab_ref.shape[1]
    u_row = lax.broadcasted_iota(jnp.int32, (n_u, n_lab), 0)
    u_col = lax.broadcasted_iota(jnp.int32, (n_u, n_lab), 1)
    lab_row = lab_ref[pl.ds(me, 1), :].astype(F32)
    lab_col = jnp.sum(jnp.where(u_row == u_col, lab_row, 0.0), axis=1, keepdims=True)
    lab_col = jnp.where(lax.broadcasted_iota(jnp.int32, (n_u, 1), 0) < n_lab, lab_col, -1.0)
    onehot_ref[...] = jnp.where(lax.broadcasted_iota(jnp.int32, (n_u, n_v), 1).astype(F32) == lab_col, 1.0, 0.0)
    bt_ref[...] = jnp.full_like(bt_ref, NEG)
    lt_ref[...] = jnp.full_like(lt_ref, NEG)
    rs_ref[...] = jnp.zeros_like(rs_ref)
    loads[4].wait()

    others = pl.ds(0, n - 1)
    pltpu.make_async_copy(abuf.at[others], arecv_buf.at[others], arecv).wait()

    def widen(b, c):
        both = arecv_buf[b].astype(F32)
        for k in range(tl):
            a_ref[b, k] = both[k:k + 1, :]
        return c
    lax.fori_loop(0, n, widen, 0, unroll=4)

    lane = lax.broadcasted_iota(jnp.int32, (n_u, LANES), 1)
    u_sub = lax.broadcasted_iota(jnp.int32, (n_u, LANES), 0)

    def scores(i, z_ref):
        for k in range(BLK_T):
            h_ref[pl.ds((i * BLK_T + k) * n_u, n_u), :] = jnp.tanh(a_ref[(i * BLK_T + k) // tl, (i * BLK_T + k) % tl] + c_ref[...]).astype(BF16)
        z_ref[...] = dot(h_ref[pl.ds(i * rows, rows), :], wo_ref[...], 1, 0)

    def stats(i, z_ref):
        for k in range(BLK_T):
            t = i * BLK_T + k
            zt = z_ref[k * n_u:(k + 1) * n_u, :]
            m = jnp.max(zt, axis=1, keepdims=True)
            e = jnp.exp(zt - m)
            s = jnp.sum(e, axis=1, keepdims=True)
            zl = jnp.sum(zt * onehot_ref[...], axis=1, keepdims=True)
            for q in range(n_v // LANES):
                e_ref[pl.ds(q * n_t * n_u + t * n_u, n_u), :] = e[:, q * LANES:(q + 1) * LANES]
            norm = m + jnp.log(s)
            here = lane == t
            bt_ref[...] = jnp.where(here, zt[:, :1] - norm, bt_ref[...])
            lt_ref[...] = jnp.where(here, zl - norm, lt_ref[...])
            rs_ref[...] = jnp.where(here, 1.0 / s, rs_ref[...])

    def pair(i, c):
        scores(2 * i + 1, z1_ref)
        stats(2 * i, z0_ref)
        scores(2 * i + 2, z0_ref)
        stats(2 * i + 1, z1_ref)
        return c
    scores(0, z0_ref)
    n_pair = n_blk // 2 - 1
    lax.fori_loop(0, 1, pair, 0)
    agf.ag1_start()
    lax.fori_loop(1, n_pair, pair, 0)
    scores(n_blk - 1, z1_ref)
    stats(n_blk - 2, z0_ref)
    stats(n_blk - 1, z1_ref)

    t_len = flen_ref[me]
    u_len = llen_ref[me]
    fill = jnp.full((LANES - n_u, LANES), NEG, F32)
    lt = jnp.where(u_sub == n_u - 1, NEG, lt_ref[...])
    d_id = lax.broadcasted_iota(jnp.int32, (LANES, LANES), 0)
    u_id = lax.broadcasted_iota(jnp.int32, (LANES, LANES), 1)
    t_id = d_id - u_id
    past = t_id >= t_len
    sb = jnp.concatenate([skew(bt_ref[...]), fill], axis=0).T
    sl = jnp.concatenate([skew(lt), fill], axis=0).T
    sb = jnp.where(past, jnp.where(u_id == u_len, 0.0, NEG), jnp.where(t_id < 0, NEG, sb))
    sl = jnp.where(past | (t_id < 0), NEG, sl)
    w0[0] = sb
    w0[1] = pltpu.roll(sl, 1, 1)
    row_id = lax.broadcasted_iota(jnp.int32, (1, LANES), 1)
    bound = jnp.where(row_id == u_len, 0.0, NEG).astype(F32)
    start = jnp.where(row_id == 0, 0.0, NEG).astype(F32)
    lattice((w0, w1, w2, w3), al_ref, be_ref, start, bound, LEVELS)
    logp = jnp.sum(jnp.where(row_id == 0, be_ref[0:1, :], 0.0), axis=1, keepdims=True)
    ok = (t_id >= 0) & jnp.logical_not(past) & (u_id < n_u)
    up = be_ref[1:LANES + 1, :]
    base = al_ref[:LANES, :] - logp
    gb = jnp.where(ok, jnp.exp(jnp.minimum(base + w0[0] + up, 0.0)), 0.0)
    gl = jnp.where(ok & (u_id < n_u - 1), jnp.exp(jnp.minimum(base + pltpu.roll(w0[1] + up, LANES - 1, 1), 0.0)), 0.0)
    gb = unskew(gb.T[:n_u])
    gl = unskew(gl.T[:n_u])
    gb_ref[...] = gb
    gl_ref[...] = gl
    c1_ref[...] = (gb + gl) * rs_ref[...]

    dc_ref[core] = jnp.zeros(dc_ref.shape[1:], F32)
    dc_ref[core, n_u:n_u + 1, :] = jnp.broadcast_to(-logp, (1, n_j))
    v0 = lax.broadcasted_iota(jnp.int32, (n_u, LANES), 1) == 0

    def grad_logits(i):
        turn = (LANES - i * BLK_T) % LANES
        c1 = pltpu.roll(c1_ref[...], turn, 1)
        gbr = pltpu.roll(gb_ref[...], turn, 1)
        glr = pltpu.roll(gl_ref[...], turn, 1)
        for k in range(BLK_T):
            at = (i * BLK_T + k) * n_u
            for q in range(n_v // LANES):
                cols = slice(q * LANES, (q + 1) * LANES)
                dz = e_ref[q * n_t * n_u + at:q * n_t * n_u + at + n_u, :] * c1[:, k:k + 1] - glr[:, k:k + 1] * onehot_ref[:, cols]
                if q == 0:
                    dz = dz - jnp.where(v0, gbr[:, k:k + 1], 0.0)
                dz_ref[at:at + n_u, cols] = dz.astype(BF16)

    def grad_out(i):
        at = slice(i * BLK_G * rows, (i + 1) * BLK_G * rows)
        r = dot(h_ref[at, :], dz_ref[at, :], 0, 0)
        for q in range(n_v // LANES):
            part = r[:, q * LANES:(q + 1) * LANES]
            p_out[q * n_j:(q + 1) * n_j] = part if i == 0 else p_out[q * n_j:(q + 1) * n_j] + part

    def grad_hidden(i, z_ref):
        z_ref[:, :n_j] = dot(dz_ref[pl.ds(i * rows, rows), :], wo_ref[...], 1, 1)

    def grad_pre(i, z_ref):
        row = []
        for k in range(BLK_T):
            t = i * BLK_T + k
            hf = h_ref[pl.ds(t * n_u, n_u), :].astype(F32)
            dpt = (z_ref[k * n_u:(k + 1) * n_u, :n_j] * (1.0 - hf * hf)).astype(BF16).astype(F32)
            row.append(jnp.sum(dpt, axis=0, keepdims=True))
            if len(row) == tl:
                dabuf[t // tl] = jnp.concatenate(row, axis=0).astype(BF16)
                row = []
            dc_ref[core, :n_u, :] += dpt

    def phase3(i, c):
        grad_hidden(2 * i + 1, z1_ref)
        grad_pre(2 * i, z0_ref)
        grad_hidden(2 * i + 2, z0_ref)
        grad_pre(2 * i + 1, z1_ref)
        return c

    for k in range(BLK_G):
        grad_logits(k)
    agf.ag1_mid()
    for i in range(n_blk // BLK_G):
        grad_out(i)
        if i + 1 < n_blk // BLK_G:
            for k in range(BLK_G):
                grad_logits(BLK_G * (i + 1) + k)
    aro.d2d_start()
    grad_hidden(0, z0_ref)
    lax.fori_loop(0, 1, phase3, 0)
    aro.rs1_start()
    agf.d2d_back()
    lax.fori_loop(1, n_pair, phase3, 0)
    grad_hidden(n_blk - 1, z1_ref)
    grad_pre(n_blk - 2, z0_ref)
    grad_pre(n_blk - 1, z1_ref)

    own_dc = dc_ref.at[core]
    dc_copy = comm.send(own_dc, own_dc, aro.sibling)
    darecv[me] = dabuf[me]
    aro.rs1_mid()

    def d_copy(p):
        to = (me + p) % n
        return pltpu.make_async_remote_copy(src_ref=dabuf.at[to], dst_ref=darecv.at[me], send_sem=dsend, recv_sem=drecv, device_id={'seq': to}, device_id_type=pl.DeviceIdType.MESH)

    def d_go(p, c):
        d_copy(p).start()
        return c
    lax.fori_loop(1, n, d_go, 0)

    dc_copy.wait_recv()
    n_g = g_ref.shape[2]
    gwp = dot(g_ref[...].reshape(2 * n_u, n_g), dc_ref[:, :n_u, :].reshape(2 * n_u, n_j).astype(BF16), 0, 0)
    for q in range(n_j // LANES):
        p_pred[q * n_g:(q + 1) * n_g] = gwp[:, q * LANES:(q + 1) * LANES]
    used = n_g * n_j // LANES
    spare = lax.broadcasted_iota(jnp.int32, (p_pred.shape[0] - used, LANES), 0) - me + core
    p_pred[used:] = jnp.where(spare == 0, dc_ref[0, n_u:n_u + 1, :LANES], jnp.where(spare == 1, dc_ref[1, n_u:n_u + 1, :LANES], 0.0))
    arp.rs1_start()
    aro.rs2_start()
    pltpu.make_async_copy(dabuf.at[others], darecv.at[others], drecv).wait()

    dal = jnp.concatenate([darecv[:, k, :] for k in range(tl)], axis=0)
    for k in range(2):
        agd.mine(k)[...] = dal[k * n:(k + 1) * n, :]
    agd.gather_start()
    arp.rs1_mid()
    aro.rs2_mid()
    agd.ag2_mid()
    genc = dot(dal, we_ref[...], 1, 1).astype(BF16)
    for k in range(tl):
        genc_out[:, k, :] = genc[k * n:(k + 1) * n, :]
    arp.rs2_start()
    aro.ag2_start()
    agd.ag1_start()
    aro.ag2_mid()
    arp.ag2_start()
    agd.ag1_mid()
    aro.ag1_start()
    arp.ag1_start()
    agd.d2d_back()

    blk = n_e // 4

    def enc_block(i, side, first):
        fb = fg_ref[side, :, :, :, :, pl.ds(pl.multiple_of(i * blk, blk), blk)].reshape(n * n_t // 2, blk)
        r = dot(fb, dg_ref[side].reshape(n * n_t // 2, n_j), 0, 0)
        at = pl.ds(pl.multiple_of(i * blk, blk), blk)
        gwe_out[at, :] = r if first else gwe_out[at, :] + r

    def enc_own(i, c):
        enc_block(i, core, True)
        return c

    def enc_other(i, c):
        enc_block(i, 1 - core, False)
        return c

    def put_cols(base, n_r, dst):
        for q in range(dst.shape[1] // LANES):
            dst[:, q * LANES:(q + 1) * LANES] = e_ref[base + q * n_r:base + (q + 1) * n_r]
    lax.fori_loop(0, 4, enc_own, 0)
    aro.ag1_mid()
    agf.finish()
    agd.finish()
    lax.fori_loop(0, 2, enc_other, 0)
    arp.ag1_mid()
    lax.fori_loop(2, 4, enc_other, 0)
    aro.d2d_back()
    arp.d2d_back()
    aro.finish()
    put_cols(0, n_j, gwo_out)
    arp.finish()
    put_cols(at_p, n_g, gwp_out)
    diag = lax.broadcasted_iota(jnp.int32, (n, n), 0) == lax.broadcasted_iota(jnp.int32, (n, n), 1)
    loss_out[...] = jnp.sum(jnp.where(diag, e_ref[at_p + used:at_p + used + n, :n], 0.0), axis=0, keepdims=True)
    pltpu.make_async_copy(abuf.at[others], arecv_buf.at[others], asend).wait()
    pltpu.make_async_copy(dabuf.at[others], darecv.at[others], dsend).wait()
    comm.drain()


def move(count, *refs):
    src, dst, sem = refs[:count], refs[count:2 * count], refs[2 * count]
    copies = [pltpu.make_async_copy(a, b, sem.at[k]) for k, (a, b) in enumerate(zip(src, dst))]
    for cp in copies:
        cp.start()
    for cp in copies:
        cp.wait()


def solution(mesh):
    n = mesh.shape['seq']
    assert n == 2 * SIDE * SIDE
    parts = 2 * n

    def local_fn(enc_out, pred_out, w_enc, w_pred, w_out, labels, frame_len, label_len):
        n_utt, n_loc, n_e = enc_out.shape
        _, n_u, n_g = pred_out.shape
        n_j, n_v = w_out.shape
        n_t = n_loc * n
        assert n_utt == n
        m_o, m_p = pieces_rows(n_j, n_v, parts), pieces_rows(n_g, n_j, parts)
        assert parts * m_p >= n_g * n_j // LANES + n
        vm = pl.BlockSpec(memory_space=pltpu.VMEM)
        sm = pl.BlockSpec(memory_space=pltpu.SMEM)
        hbm = pl.BlockSpec(memory_space=pl.ANY)

        def ar_scratch(m):
            return [pltpu.VMEM((2, 6, 2, m, LANES), F32), pltpu.VMEM((2, 6, m, LANES), F32)]
        hf = pltpu.VMEM((n_u, LANES), F32)
        n_sem = 42 + 33 + 17 + 15 + 1
        row = pltpu.VMEM((n, n_loc, 1, n_j), F32)
        msg = pltpu.VMEM((n, n_loc, n_j), BF16)
        levels = [pltpu.VMEM((2 ** lv + 1, LANES >> lv, LANES), F32) for lv in range(LEVELS + 1)]
        shapes = tuple(jax.ShapeDtypeStruct(*a) for a in (((1, n), F32), ((n_utt, n_loc, n_e), BF16), ((n_e, n_j), F32), ((n_g, n_j), F32), ((n_j, n_v), F32)))
        outs = pl.pallas_call(
            functools.partial(kernel, n),
            out_shape=tuple(pltpu.VMEM(o.shape, o.dtype) for o in shapes),
            in_specs=[hbm, hbm, hbm, hbm, hbm, vm, sm, sm],
            out_specs=(vm,) * 5,
            scratch_shapes=[
                pltpu.VMEM((n_utt, n_loc, n_e), BF16), pltpu.VMEM((n_e, n_j), BF16), pltpu.VMEM((n_g, n_j), BF16), pltpu.VMEM((n_j, n_v), BF16),
                pltpu.VMEM((2, n_u, n_g), BF16), msg, msg, row,
                pltpu.VMEM((n_u, n_j), F32), pltpu.VMEM((n_u, n_v), F32), pltpu.VMEM((n_t * n_u, n_j), BF16),
                pltpu.VMEM((BLK_T * n_u, n_v), F32), pltpu.VMEM((BLK_T * n_u, n_v), F32),
                pltpu.VMEM((n_t * n_u * n_v // LANES, LANES), F32), hf, hf, hf,
                *levels, pltpu.VMEM((LANES + 8, LANES), F32), pltpu.VMEM((LANES + 8, LANES), F32), hf, hf, hf,
                pltpu.VMEM((n_t * n_u, n_v), BF16), pltpu.VMEM((2, n_u + 8, n_j), F32),
                msg, msg,
                pltpu.VMEM((2, 2, SIDE, SIDE, n, n_e), BF16), pltpu.VMEM((2, 2, SIDE, SIDE, n, n_j), BF16),
                pltpu.VMEM((parts * m_o, LANES), F32),
                pltpu.VMEM((2, SIDE, SIDE, m_o, LANES), F32), *ar_scratch(m_o), *ar_scratch(m_p),
                pltpu.SemaphoreType.DMA((5,)),
                pltpu.SemaphoreType.DMA, pltpu.SemaphoreType.DMA, pltpu.SemaphoreType.DMA, pltpu.SemaphoreType.DMA,
                pltpu.SemaphoreType.DMA((48,)), pltpu.SemaphoreType.DMA((n_sem,))],
            compiler_params=pltpu.CompilerParams(collective_id=0, has_side_effects=True, vmem_limit_bytes=57 * 1024 * 1024 - 128 * 1024),
        )(enc_out, pred_out, w_enc, w_pred, w_out, labels, frame_len, label_len)
        loss, genc, gwe, gwp, gwo = pl.pallas_call(
            functools.partial(move, len(shapes)), out_shape=shapes, in_specs=[vm] * len(shapes), out_specs=(hbm,) * len(shapes),
            scratch_shapes=[pltpu.SemaphoreType.DMA((len(shapes),))], compiler_params=pltpu.CompilerParams(vmem_limit_bytes=256 * 1024))(*outs)
        return loss.reshape(n), genc, gwe, gwp, gwo

    in_specs = (P('dp', 'seq', None), P('dp', None, None), P(None, None), P(None, None), P(None, None), P('dp', None), P('dp'), P('dp'))
    out_specs = (P('dp'), P('dp', 'seq', None), P('dp', None), P('dp', None), P('dp', None))
    return jax.shard_map(local_fn, mesh=mesh, in_specs=in_specs, out_specs=out_specs, check_vma=False)
```

```python
import functools

import jax
import jax.numpy as jnp
from jax import lax
from jax.experimental import pallas as pl
from jax.experimental.pallas import tpu as pltpu
from jax.sharding import PartitionSpec as P

NEG = -1.0e30
SIDE = 4
LANES = 128
BLK_T = 8
F32 = jnp.float32
BF16 = jnp.bfloat16


def dot(a, b, ca, cb):
    return lax.dot_general(a, b, (((ca,), (cb,)), ((), ())), preferred_element_type=F32)


def lse2(x, y):
    m = jnp.maximum(x, y)
    return m + jnp.log(1.0 + jnp.exp(-jnp.abs(x - y)))


def pieces_rows(rows, cols, parts):
    tiles = rows * cols // (8 * LANES)
    return -(-tiles // parts) * 8


class Comm:
    def __init__(self, send_sem, recv_sem):
        self.send_sem, self.recv_sem, self.used, self.sent = send_sem, recv_sem, 0, {}

    def send(self, src, dst, dev):
        k, slot = self.used, self.used % self.send_sem.shape[0]
        self.used += 1
        if slot in self.sent:
            self.sent.pop(slot).wait_send()
        cp = pltpu.make_async_remote_copy(src_ref=src, dst_ref=dst, send_sem=self.send_sem.at[slot], recv_sem=self.recv_sem.at[k],
                                          device_id={'seq': dev}, device_id_type=pl.DeviceIdType.MESH)
        cp.start()
        self.sent[slot] = cp
        return cp

    def drain(self):
        for cp in self.sent.values():
            cp.wait_send()
        self.sent = {}


class Ring:
    def __init__(self, pos, dev_of):
        self.me, self.r, self.l, self.o = pos, (pos + 1) % SIDE, (pos + 3) % SIDE, (pos + 2) % SIDE
        self.right, self.left, self.opp = dev_of(self.r), dev_of(self.l), dev_of(self.o)


def rs_start(comm, ring, view, buf):
    return (comm.send(view(ring.o, 0), buf[0], ring.right), comm.send(view(ring.o, 1), buf[2], ring.left),
            comm.send(view(ring.r, 1), buf[1], ring.right), comm.send(view(ring.l, 0), buf[3], ring.left))


def rs_mid(comm, ring, view, buf, st):
    st[0].wait_recv()
    v = view(ring.r, 0)
    v[...] += buf[0][...]
    a = comm.send(v, buf[4], ring.right)
    st[1].wait_recv()
    v = view(ring.l, 1)
    v[...] += buf[2][...]
    b = comm.send(v, buf[5], ring.left)
    return st + (a, b)


def rs_end(ring, view, buf, st, out):
    for k in (2, 3, 4, 5):
        st[k].wait_recv()
    out(0, view(ring.me, 0)[...] + buf[4][...] + buf[3][...])
    out(1, view(ring.me, 1)[...] + buf[5][...] + buf[1][...])


def ex_start(comm, ring, view, buf):
    return tuple(comm.send(view(at), b, to) for at, b, to in zip((ring.r, ring.l, ring.o), buf, (ring.right, ring.left, ring.opp)))


def ag_start(comm, ring, whole):
    v = whole(ring.me)
    return (comm.send(v, v, ring.right), comm.send(v, v, ring.left))


def ag_mid(comm, ring, half, st):
    st[0].wait_recv()
    v = half(ring.l, 0)
    a = comm.send(v, v, ring.right)
    st[1].wait_recv()
    v = half(ring.r, 1)
    b = comm.send(v, v, ring.left)
    return (a, b)


def ag_end(st):
    st[0].wait_recv()
    st[1].wait_recv()


class AllReduce:
    def __init__(self, comm, pos, full, part=None, r0=None, r1=None, r2=None, relay=False):
        self.comm, (self.core, x, y, dev) = comm, pos
        self.part, self.full, self.r0, self.r1, self.r2, self.relay = part, full, r0, r1, r2, relay
        rx = Ring(x, lambda i: dev(i, y, self.core))
        ry = Ring(y, lambda i: dev(x, i, self.core))
        self.rings = ((rx, ry), (ry, rx))
        self.sibling = dev(x, y, 1 - self.core)
        n = full.shape[4]
        self.spans = ((0, n // 32 * 16), (n // 32 * 16, n - n // 32 * 16))

    def v1(self, ref, k):
        return lambda a, half: ref.at[self.core, k, a, pl.ds(2 * half, 2)]

    def v2(self, ref, k):
        return lambda b: ref.at[self.core, k, self.rings[k][0].me, b]

    def v2h(self, ref, k):
        return lambda b, half: ref.at[self.core, k, self.rings[k][0].me, b, pl.ds(*self.spans[half])]

    def b1(self, k):
        return [self.r1.at[k, s] for s in range(6)]

    def b2(self, k):
        return [self.r2.at[k, s] for s in range(3)]

    def b2h(self, k):
        return [self.r2.at[k, s, pl.ds(*self.spans[half])] for s, half in enumerate((0, 1, 1, 0, 0, 1))]

    def mine(self, k):
        return self.full.at[self.core, k, self.rings[k][0].me, self.rings[k][1].me]

    def d2d_start(self):
        self.st0 = self.comm.send(self.part.at[1 - self.core], self.r0, self.sibling)

    def rs1_start(self):
        if self.r0 is not None:
            self.st0.wait_recv()
            self.part[pl.ds(self.core, 1)] += self.r0[...][None]
        self.st = [rs_start(self.comm, self.rings[k][0], self.v1(self.part, k), self.b1(k)) for k in range(2)]

    def rs1_mid(self):
        self.st = [rs_mid(self.comm, self.rings[k][0], self.v1(self.part, k), self.b1(k), self.st[k]) for k in range(2)]

    def rs2_start(self):
        for k in range(2):
            view = self.v1(self.part, k)

            def put(half, val, view=view, k=k):
                view(self.rings[k][0].me, half)[...] = val
            rs_end(self.rings[k][0], view, self.b1(k), self.st[k], put)
            if self.relay:
                self.st[k] = rs_start(self.comm, self.rings[k][1], self.v2h(self.part, k), self.b2h(k))
            else:
                self.st[k] = ex_start(self.comm, self.rings[k][1], self.v2(self.part, k), self.b2(k))

    def rs2_mid(self):
        self.st = [rs_mid(self.comm, self.rings[k][1], self.v2h(self.part, k), self.b2h(k), self.st[k]) for k in range(2)]

    def ag2_start(self):
        for k in range(2):
            if self.relay:
                dst = self.v2h(self.full, k)

                def put(half, val, dst=dst, k=k):
                    dst(self.rings[k][1].me, half)[...] = val
                rs_end(self.rings[k][1], self.v2h(self.part, k), self.b2h(k), self.st[k], put)
            else:
                for cp in self.st[k]:
                    cp.wait_recv()
                got = self.b2(k)
                self.mine(k)[...] = self.v2(self.part, k)(self.rings[k][1].me)[...] + got[0][...] + got[1][...] + got[2][...]
        self.gather_start()

    def gather_start(self):
        self.st = []
        for k in range(2):
            own, ring = self.mine(k), self.rings[k][1]
            if self.relay:
                self.st.append((self.comm.send(own, own, ring.right), self.comm.send(own, own, ring.left)))
            else:
                self.st.append(ex_start(self.comm, ring, lambda b, own=own: own, (own, own, own)))

    def ag2_mid(self):
        self.st = [ag_mid(self.comm, self.rings[k][1], self.v2h(self.full, k), self.st[k]) for k in range(2)]

    def ag1_start(self):
        for k in range(2):
            for cp in self.st[k]:
                cp.wait_recv()
            self.st[k] = ag_start(self.comm, self.rings[k][0], lambda a, k=k: self.full.at[self.core, k, a])

    def ag1_mid(self):
        self.st = [ag_mid(self.comm, self.rings[k][0], self.v1(self.full, k), self.st[k]) for k in range(2)]

    def d2d_back(self):
        for k in range(2):
            ag_end(self.st[k])
        half = self.full.at[self.core]
        self.st0 = self.comm.send(half, half, self.sibling)

    def finish(self):
        self.st0.wait_recv()


def skew(mat):
    return pltpu.roll(mat, 0, 1, stride=1, stride_axis=0)


def unskew(mat):
    rows = lax.broadcasted_iota(jnp.int32, mat.shape, 0)
    bit = 1
    while bit < mat.shape[0]:
        mat = jnp.where((rows & bit) != 0, pltpu.roll(mat, LANES - bit, 1), mat)
        bit *= 2
    return mat


def lse(terms):
    m = functools.reduce(jnp.maximum, terms)
    return m + jnp.log(functools.reduce(jnp.add, [jnp.exp(x - m) for x in terms]))


def shift(x, k):
    return x if k == 0 else pltpu.roll(x, k % LANES, 1)


def compose(first, second):
    r = len(first) - 1
    return [lse([shift(first[k - j], j) + second[j] for j in range(max(0, k - r), min(r, k) + 1)]) for k in range(2 * r + 1)]


def every(ref, k, start, step):
    return ref[k, pl.ds(start, LANES // step, stride=step), :]


def lattice(w_refs, al_ref, be_ref, start, bound, levels):
    for lv in range(levels):
        src, dst, rows = w_refs[lv], w_refs[lv + 1], LANES >> lv
        r = 2 ** lv
        first = [src[k, pl.ds(0, rows // 2, stride=2), :] for k in range(r + 1)]
        second = [src[k, pl.ds(1, rows // 2, stride=2), :] for k in range(r + 1)]
        for k, w in enumerate(compose(first, second)):
            dst[k, :rows // 2, :] = w
    hop = 2 ** levels
    top, n_hop = w_refs[levels], LANES // hop
    al_ref[0:1, :] = start
    be_ref[LANES:LANES + 8, :] = jnp.broadcast_to(bound, (8, LANES))

    def chain(i, carry):
        alpha, beta = carry
        j = n_hop - 1 - i
        alpha = lse([shift(alpha, k) + top[k, pl.ds(i, 1), :] for k in range(hop + 1)])
        beta = lse([shift(beta + top[k, pl.ds(j, 1), :], -k) for k in range(hop + 1)])
        al_ref[pl.ds((i + 1) * hop, 1), :] = alpha
        be_ref[pl.ds(j * hop, 1), :] = beta
        return alpha, beta
    lax.fori_loop(0, n_hop, chain, (start, bound))
    for lv in range(levels - 1, -1, -1):
        r = 2 ** lv
        n_r = LANES // (2 * r)
        al = al_ref[pl.ds(0, n_r, stride=2 * r), :]
        be = be_ref[pl.ds(2 * r, n_r, stride=2 * r), :]
        al_ref[pl.ds(r, n_r, stride=2 * r), :] = lse([shift(al, k) + w_refs[lv][k, pl.ds(0, n_r, stride=2), :] for k in range(r + 1)])
        be_ref[pl.ds(r, n_r, stride=2 * r), :] = lse([shift(be + w_refs[lv][k, pl.ds(1, n_r, stride=2), :], -k) for k in range(r + 1)])


LEVELS = 3
MOVE_PARTS = 4
BLK_G = 2


def kernel(n, f_hbm, pred_ref, we_hbm, wp_hbm, wo_hbm, lab_ref, flen_ref, llen_ref,
           loss_out, genc_out, gwe_out, gwp_out, gwo_out,
           f_ref, we_ref, wp_ref, wo_ref, g_ref, abuf, arecv_buf, a_ref, c_ref, onehot_ref, h_ref, z0_ref, z1_ref, e_ref, bt_ref, lt_ref, rs_ref,
           w0, w1, w2, w3, al_ref, be_ref, c1_ref, gb_ref, gl_ref, dz_ref, dc_ref, dabuf, darecv,
           fg_ref, dg_ref, p_out, r0a, r1a, r2a, r1p, r2p,
           insem, asend, arecv, dsend, drecv, ssem, rsem):
    me = lax.axis_index('seq')
    core, x, y = me % 2, (me // 2) % SIDE, me // (2 * SIDE)

    def dev(i, j, c):
        return (j * SIDE + i) * 2 + c

    n_t, n_u, n_j, n_v = n * a_ref.shape[1], c_ref.shape[0], c_ref.shape[1], wo_ref.shape[1]
    n_e = f_ref.shape[2]
    tl = n_t // n
    rows = BLK_T * n_u
    n_blk = n_t // BLK_T

    barrier = pltpu.get_barrier_semaphore()

    loads = [pltpu.make_async_copy(src, dst, insem.at[k]) for k, (src, dst) in enumerate(
        ((f_hbm, f_ref), (we_hbm, we_ref), (pred_ref.at[pl.ds(me - core, 2)], g_ref), (wp_hbm, wp_ref), (wo_hbm, wo_ref)))]
    for cp in loads:
        cp.start()
    def greet(p, c):
        pl.semaphore_signal(barrier, inc=1, device_id={'seq': (me + p) % n}, device_id_type=pl.DeviceIdType.MESH)
        return c
    lax.fori_loop(1, n, greet, 0)
    comm = Comm(ssem, rsem)
    pos = (core, x, y, dev)

    def six(ref, base, m):
        return ref.at[pl.ds(base, 64 * m)].reshape(2, 2, SIDE, SIDE, m, LANES)
    m_o = n_j * n_v // LANES // 64
    m_p = r2p.shape[2]
    at_p = 64 * m_o
    p_pred = e_ref.at[pl.ds(at_p + 64 * m_p, 64 * m_p)]
    aro = AllReduce(comm, pos, six(e_ref, 0, m_o), six(p_out, 0, m_o), r0a, r1a, r2a, relay=True)
    arp = AllReduce(comm, pos, six(e_ref, at_p, m_p), six(e_ref, at_p + 64 * m_p, m_p), None, r1p, r2p)
    agf = AllReduce(comm, pos, fg_ref)
    agd = AllReduce(comm, pos, dg_ref, relay=True)

    loads[0].wait()
    loads[1].wait()
    for k in range(tl):
        agf.mine(k)[...] = f_ref[:, k, :]
    f_loc = jnp.concatenate([agf.mine(k)[...] for k in range(tl)], axis=0)
    act = dot(f_loc, we_ref[...], 1, 0).astype(BF16)
    for k in range(tl):
        abuf[:, k, :] = act[k * n:(k + 1) * n, :]
    arecv_buf[me] = abuf[me]
    pl.semaphore_wait(barrier, n - 1)

    def a_copy(p):
        to = (me + p) % n
        return pltpu.make_async_remote_copy(src_ref=abuf.at[to], dst_ref=arecv_buf.at[me], send_sem=asend, recv_sem=arecv, device_id={'seq': to}, device_id_type=pl.DeviceIdType.MESH)

    def a_go(p, c):
        a_copy(p).start()
        return c
    lax.fori_loop(1, n, a_go, 0)
    agf.gather_start()

    loads[2].wait()
    loads[3].wait()
    c_ref[...] = dot(g_ref[core], wp_ref[...], 1, 0).astype(BF16).astype(F32)
    n_lab = lab_ref.shape[1]
    u_row = lax.broadcasted_iota(jnp.int32, (n_u, n_lab), 0)
    u_col = lax.broadcasted_iota(jnp.int32, (n_u, n_lab), 1)
    lab_row = lab_ref[pl.ds(me, 1), :].astype(F32)
    lab_col = jnp.sum(jnp.where(u_row == u_col, lab_row, 0.0), axis=1, keepdims=True)
    lab_col = jnp.where(lax.broadcasted_iota(jnp.int32, (n_u, 1), 0) < n_lab, lab_col, -1.0)
    onehot_ref[...] = jnp.where(lax.broadcasted_iota(jnp.int32, (n_u, n_v), 1).astype(F32) == lab_col, 1.0, 0.0)
    bt_ref[...] = jnp.full_like(bt_ref, NEG)
    lt_ref[...] = jnp.full_like(lt_ref, NEG)
    rs_ref[...] = jnp.zeros_like(rs_ref)
    loads[4].wait()

    others = pl.ds(0, n - 1)
    pltpu.make_async_copy(abuf.at[others], arecv_buf.at[others], arecv).wait()

    def widen(b, c):
        both = arecv_buf[b].astype(F32)
        for k in range(tl):
            a_ref[b, k] = both[k:k + 1, :]
        return c
    lax.fori_loop(0, n, widen, 0, unroll=4)

    lane = lax.broadcasted_iota(jnp.int32, (n_u, LANES), 1)
    u_sub = lax.broadcasted_iota(jnp.int32, (n_u, LANES), 0)

    def scores(i, z_ref):
        for k in range(BLK_T):
            h_ref[pl.ds((i * BLK_T + k) * n_u, n_u), :] = jnp.tanh(a_ref[(i * BLK_T + k) // tl, (i * BLK_T + k) % tl] + c_ref[...]).astype(BF16)
        z_ref[...] = dot(h_ref[pl.ds(i * rows, rows), :], wo_ref[...], 1, 0)

    def stats(i, z_ref):
        for k in range(BLK_T):
            t = i * BLK_T + k
            zt = z_ref[k * n_u:(k + 1) * n_u, :]
            m = jnp.max(zt, axis=1, keepdims=True)
            e = jnp.exp(zt - m)
            s = jnp.sum(e, axis=1, keepdims=True)
            zl = jnp.sum(zt * onehot_ref[...], axis=1, keepdims=True)
            for q in range(n_v // LANES):
                e_ref[pl.ds(q * n_t * n_u + t * n_u, n_u), :] = e[:, q * LANES:(q + 1) * LANES]
            norm = m + jnp.log(s)
            here = lane == t
            bt_ref[...] = jnp.where(here, zt[:, :1] - norm, bt_ref[...])
            lt_ref[...] = jnp.where(here, zl - norm, lt_ref[...])
            rs_ref[...] = jnp.where(here, 1.0 / s, rs_ref[...])

    def pair(i, c):
        scores(2 * i + 1, z1_ref)
        stats(2 * i, z0_ref)
        scores(2 * i + 2, z0_ref)
        stats(2 * i + 1, z1_ref)
        return c
    scores(0, z0_ref)
    n_pair = n_blk // 2 - 1
    lax.fori_loop(0, 1, pair, 0)
    agf.ag1_start()
    lax.fori_loop(1, n_pair, pair, 0)
    scores(n_blk - 1, z1_ref)
    stats(n_blk - 2, z0_ref)
    stats(n_blk - 1, z1_ref)

    t_len = flen_ref[me]
    u_len = llen_ref[me]
    fill = jnp.full((LANES - n_u, LANES), NEG, F32)
    lt = jnp.where(u_sub == n_u - 1, NEG, lt_ref[...])
    d_id = lax.broadcasted_iota(jnp.int32, (LANES, LANES), 0)
    u_id = lax.broadcasted_iota(jnp.int32, (LANES, LANES), 1)
    t_id = d_id - u_id
    past = t_id >= t_len
    sb = jnp.concatenate([skew(bt_ref[...]), fill], axis=0).T
    sl = jnp.concatenate([skew(lt), fill], axis=0).T
    sb = jnp.where(past, jnp.where(u_id == u_len, 0.0, NEG), jnp.where(t_id < 0, NEG, sb))
    sl = jnp.where(past | (t_id < 0), NEG, sl)
    w0[0] = sb
    w0[1] = pltpu.roll(sl, 1, 1)
    row_id = lax.broadcasted_iota(jnp.int32, (1, LANES), 1)
    bound = jnp.where(row_id == u_len, 0.0, NEG).astype(F32)
    start = jnp.where(row_id == 0, 0.0, NEG).astype(F32)
    lattice((w0, w1, w2, w3), al_ref, be_ref, start, bound, LEVELS)
    logp = jnp.sum(jnp.where(row_id == 0, be_ref[0:1, :], 0.0), axis=1, keepdims=True)
    ok = (t_id >= 0) & jnp.logical_not(past) & (u_id < n_u)
    up = be_ref[1:LANES + 1, :]
    base = al_ref[:LANES, :] - logp
    gb = jnp.where(ok, jnp.exp(jnp.minimum(base + w0[0] + up, 0.0)), 0.0)
    gl = jnp.where(ok & (u_id < n_u - 1), jnp.exp(jnp.minimum(base + pltpu.roll(w0[1] + up, LANES - 1, 1), 0.0)), 0.0)
    gb = unskew(gb.T[:n_u])
    gl = unskew(gl.T[:n_u])
    gb_ref[...] = gb
    gl_ref[...] = gl
    c1_ref[...] = (gb + gl) * rs_ref[...]

    dc_ref[core] = jnp.zeros(dc_ref.shape[1:], F32)
    dc_ref[core, n_u:n_u + 1, :] = jnp.broadcast_to(-logp, (1, n_j))
    v0 = lax.broadcasted_iota(jnp.int32, (n_u, LANES), 1) == 0

    def grad_logits(i):
        turn = (LANES - i * BLK_T) % LANES
        c1 = pltpu.roll(c1_ref[...], turn, 1)
        gbr = pltpu.roll(gb_ref[...], turn, 1)
        glr = pltpu.roll(gl_ref[...], turn, 1)
        for k in range(BLK_T):
            at = (i * BLK_T + k) * n_u
            for q in range(n_v // LANES):
                cols = slice(q * LANES, (q + 1) * LANES)
                dz = e_ref[q * n_t * n_u + at:q * n_t * n_u + at + n_u, :] * c1[:, k:k + 1] - glr[:, k:k + 1] * onehot_ref[:, cols]
                if q == 0:
                    dz = dz - jnp.where(v0, gbr[:, k:k + 1], 0.0)
                dz_ref[at:at + n_u, cols] = dz.astype(BF16)

    def grad_out(i):
        at = slice(i * BLK_G * rows, (i + 1) * BLK_G * rows)
        r = dot(h_ref[at, :], dz_ref[at, :], 0, 0)
        for q in range(n_v // LANES):
            part = r[:, q * LANES:(q + 1) * LANES]
            p_out[q * n_j:(q + 1) * n_j] = part if i == 0 else p_out[q * n_j:(q + 1) * n_j] + part

    def grad_hidden(i, z_ref):
        z_ref[:, :n_j] = dot(dz_ref[pl.ds(i * rows, rows), :], wo_ref[...], 1, 1)

    def grad_pre(i, z_ref):
        row = []
        for k in range(BLK_T):
            t = i * BLK_T + k
            hf = h_ref[pl.ds(t * n_u, n_u), :].astype(F32)
            dpt = (z_ref[k * n_u:(k + 1) * n_u, :n_j] * (1.0 - hf * hf)).astype(BF16).astype(F32)
            row.append(jnp.sum(dpt, axis=0, keepdims=True))
            if len(row) == tl:
                dabuf[t // tl] = jnp.concatenate(row, axis=0).astype(BF16)
                row = []
            dc_ref[core, :n_u, :] += dpt

    def phase3(i, c):
        grad_hidden(2 * i + 1, z1_ref)
        grad_pre(2 * i, z0_ref)
        grad_hidden(2 * i + 2, z0_ref)
        grad_pre(2 * i + 1, z1_ref)
        return c

    for k in range(BLK_G):
        grad_logits(k)
    agf.ag1_mid()
    for i in range(n_blk // BLK_G):
        grad_out(i)
        if i + 1 < n_blk // BLK_G:
            for k in range(BLK_G):
                grad_logits(BLK_G * (i + 1) + k)
    aro.d2d_start()
    grad_hidden(0, z0_ref)
    lax.fori_loop(0, 1, phase3, 0)
    aro.rs1_start()
    agf.d2d_back()
    lax.fori_loop(1, n_pair, phase3, 0)
    grad_hidden(n_blk - 1, z1_ref)
    grad_pre(n_blk - 2, z0_ref)
    grad_pre(n_blk - 1, z1_ref)

    own_dc = dc_ref.at[core]
    dc_copy = comm.send(own_dc, own_dc, aro.sibling)
    darecv[me] = dabuf[me]
    aro.rs1_mid()

    def d_copy(p):
        to = (me + p) % n
        return pltpu.make_async_remote_copy(src_ref=dabuf.at[to], dst_ref=darecv.at[me], send_sem=dsend, recv_sem=drecv, device_id={'seq': to}, device_id_type=pl.DeviceIdType.MESH)

    def d_go(p, c):
        d_copy(p).start()
        return c
    lax.fori_loop(1, n, d_go, 0)

    dc_copy.wait_recv()
    n_g = g_ref.shape[2]
    gwp = dot(g_ref[...].reshape(2 * n_u, n_g), dc_ref[:, :n_u, :].reshape(2 * n_u, n_j).astype(BF16), 0, 0)
    for q in range(n_j // LANES):
        p_pred[q * n_g:(q + 1) * n_g] = gwp[:, q * LANES:(q + 1) * LANES]
    used = n_g * n_j // LANES
    spare = lax.broadcasted_iota(jnp.int32, (p_pred.shape[0] - used, LANES), 0) - me + core
    p_pred[used:] = jnp.where(spare == 0, dc_ref[0, n_u:n_u + 1, :LANES], jnp.where(spare == 1, dc_ref[1, n_u:n_u + 1, :LANES], 0.0))
    arp.rs1_start()
    aro.rs2_start()
    pltpu.make_async_copy(dabuf.at[others], darecv.at[others], drecv).wait()

    dal = jnp.concatenate([darecv[:, k, :] for k in range(tl)], axis=0)
    for k in range(2):
        agd.mine(k)[...] = dal[k * n:(k + 1) * n, :]
    agd.gather_start()
    arp.rs1_mid()
    aro.rs2_mid()
    agd.ag2_mid()
    genc = dot(dal, we_ref[...], 1, 1).astype(BF16)
    for k in range(tl):
        genc_out[:, k, :] = genc[k * n:(k + 1) * n, :]
    arp.rs2_start()
    aro.ag2_start()
    agd.ag1_start()
    aro.ag2_mid()
    arp.ag2_start()
    agd.ag1_mid()
    aro.ag1_start()
    arp.ag1_start()
    agd.d2d_back()

    blk = n_e // 4

    def enc_block(i, side, first):
        fb = fg_ref[side, :, :, :, :, pl.ds(pl.multiple_of(i * blk, blk), blk)].reshape(n * n_t // 2, blk)
        r = dot(fb, dg_ref[side].reshape(n * n_t // 2, n_j), 0, 0)
        at = pl.ds(pl.multiple_of(i * blk, blk), blk)
        gwe_out[at, :] = r if first else gwe_out[at, :] + r

    def enc_own(i, c):
        enc_block(i, core, True)
        return c

    def enc_other(i, c):
        enc_block(i, 1 - core, False)
        return c

    def put_cols(base, n_r, dst):
        for q in range(dst.shape[1] // LANES):
            dst[:, q * LANES:(q + 1) * LANES] = e_ref[base + q * n_r:base + (q + 1) * n_r]
    lax.fori_loop(0, 4, enc_own, 0)
    aro.ag1_mid()
    agf.finish()
    agd.finish()
    lax.fori_loop(0, 2, enc_other, 0)
    arp.ag1_mid()
    lax.fori_loop(2, 4, enc_other, 0)
    aro.d2d_back()
    arp.d2d_back()
    aro.finish()
    put_cols(0, n_j, gwo_out)
    arp.finish()
    put_cols(at_p, n_g, gwp_out)
    diag = lax.broadcasted_iota(jnp.int32, (n, n), 0) == lax.broadcasted_iota(jnp.int32, (n, n), 1)
    loss_out[...] = jnp.sum(jnp.where(diag, e_ref[at_p + used:at_p + used + n, :n], 0.0), axis=0, keepdims=True)
    pltpu.make_async_copy(abuf.at[others], arecv_buf.at[others], asend).wait()
    pltpu.make_async_copy(dabuf.at[others], darecv.at[others], dsend).wait()
    comm.drain()


def move(count, *refs):
    src, dst, sem = refs[:count], refs[count:2 * count], refs[2 * count]
    parts = []
    for a, b in zip(src, dst):
        cut = MOVE_PARTS if len(a.shape) == 2 and a.shape[0] % (8 * MOVE_PARTS) == 0 else 1
        size = a.shape[0] // cut
        parts += [(a.at[pl.ds(k * size, size)], b.at[pl.ds(k * size, size)]) for k in range(cut)]
    copies = [pltpu.make_async_copy(a, b, sem.at[k]) for k, (a, b) in enumerate(parts)]
    for cp in copies:
        cp.start()
    for cp in copies:
        cp.wait()


def solution(mesh):
    n = mesh.shape['seq']
    assert n == 2 * SIDE * SIDE
    parts = 2 * n

    def local_fn(enc_out, pred_out, w_enc, w_pred, w_out, labels, frame_len, label_len):
        n_utt, n_loc, n_e = enc_out.shape
        _, n_u, n_g = pred_out.shape
        n_j, n_v = w_out.shape
        n_t = n_loc * n
        assert n_utt == n
        m_o, m_p = pieces_rows(n_j, n_v, parts), pieces_rows(n_g, n_j, parts)
        assert parts * m_p >= n_g * n_j // LANES + n
        vm = pl.BlockSpec(memory_space=pltpu.VMEM)
        sm = pl.BlockSpec(memory_space=pltpu.SMEM)
        hbm = pl.BlockSpec(memory_space=pl.ANY)

        def ar_scratch(m):
            return [pltpu.VMEM((2, 6, 2, m, LANES), F32), pltpu.VMEM((2, 6, m, LANES), F32)]
        hf = pltpu.VMEM((n_u, LANES), F32)
        n_sem = 42 + 33 + 17 + 15 + 1
        row = pltpu.VMEM((n, n_loc, 1, n_j), F32)
        msg = pltpu.VMEM((n, n_loc, n_j), BF16)
        levels = [pltpu.VMEM((2 ** lv + 1, LANES >> lv, LANES), F32) for lv in range(LEVELS + 1)]
        shapes = tuple(jax.ShapeDtypeStruct(*a) for a in (((1, n), F32), ((n_utt, n_loc, n_e), BF16), ((n_e, n_j), F32), ((n_g, n_j), F32), ((n_j, n_v), F32)))
        outs = pl.pallas_call(
            functools.partial(kernel, n),
            out_shape=tuple(pltpu.VMEM(o.shape, o.dtype) for o in shapes),
            in_specs=[hbm, hbm, hbm, hbm, hbm, vm, sm, sm],
            out_specs=(vm,) * 5,
            scratch_shapes=[
                pltpu.VMEM((n_utt, n_loc, n_e), BF16), pltpu.VMEM((n_e, n_j), BF16), pltpu.VMEM((n_g, n_j), BF16), pltpu.VMEM((n_j, n_v), BF16),
                pltpu.VMEM((2, n_u, n_g), BF16), msg, msg, row,
                pltpu.VMEM((n_u, n_j), F32), pltpu.VMEM((n_u, n_v), F32), pltpu.VMEM((n_t * n_u, n_j), BF16),
                pltpu.VMEM((BLK_T * n_u, n_v), F32), pltpu.VMEM((BLK_T * n_u, n_v), F32),
                pltpu.VMEM((n_t * n_u * n_v // LANES, LANES), F32), hf, hf, hf,
                *levels, pltpu.VMEM((LANES + 8, LANES), F32), pltpu.VMEM((LANES + 8, LANES), F32), hf, hf, hf,
                pltpu.VMEM((n_t * n_u, n_v), BF16), pltpu.VMEM((2, n_u + 8, n_j), F32),
                msg, msg,
                pltpu.VMEM((2, 2, SIDE, SIDE, n, n_e), BF16), pltpu.VMEM((2, 2, SIDE, SIDE, n, n_j), BF16),
                pltpu.VMEM((parts * m_o, LANES), F32),
                pltpu.VMEM((2, SIDE, SIDE, m_o, LANES), F32), *ar_scratch(m_o), *ar_scratch(m_p),
                pltpu.SemaphoreType.DMA((5,)),
                pltpu.SemaphoreType.DMA, pltpu.SemaphoreType.DMA, pltpu.SemaphoreType.DMA, pltpu.SemaphoreType.DMA,
                pltpu.SemaphoreType.DMA((32,)), pltpu.SemaphoreType.DMA((n_sem,))],
            compiler_params=pltpu.CompilerParams(collective_id=0, has_side_effects=True, vmem_limit_bytes=57 * 1024 * 1024 - 128 * 1024),
        )(enc_out, pred_out, w_enc, w_pred, w_out, labels, frame_len, label_len)
        loss, genc, gwe, gwp, gwo = pl.pallas_call(
            functools.partial(move, len(shapes)), out_shape=shapes, in_specs=[vm] * len(shapes), out_specs=(hbm,) * len(shapes),
            scratch_shapes=[pltpu.SemaphoreType.DMA((MOVE_PARTS * len(shapes),))], compiler_params=pltpu.CompilerParams(vmem_limit_bytes=256 * 1024))(*outs)
        return loss.reshape(n), genc, gwe, gwp, gwo

    in_specs = (P('dp', 'seq', None), P('dp', None, None), P(None, None), P(None, None), P(None, None), P('dp', None), P('dp'), P('dp'))
    out_specs = (P('dp'), P('dp', 'seq', None), P('dp', None), P('dp', None), P('dp', None))
    return jax.shard_map(local_fn, mesh=mesh, in_specs=in_specs, out_specs=out_specs, check_vma=False)
```
